8 devices in a mesh: frag: 1 (over z), dev2: 2 (over y), dev: 4 (over x, core).
Axes of the slice: x: 2, y: 2, z: 1, core: 2. Of those that a mesh axis runs over, the one named last changes fastest.
Arguments:
- ao_ints: bfloat16 [116, 116, 116, 116], P(('frag', 'dev'), 'dev2')
- c_occ: bfloat16 [116, 6], P('frag')
- c_vir: bfloat16 [116, 112], P('frag')
Outputs:
- output: float32 [6, 112, 672], P(None, None, ('frag', 'dev2', 'dev'))
All inputs are finite; a program needn't handle non-finite values.
Results may differ from the reference program's by a relative error of at most 0.001.
Values are sent between devices in bfloat16 or wider.
A program may use at most 1 GiB of HBM per device.

```python
import jax
import jax.numpy as jnp
from jax import lax

N_BASIS = 116
N_OCC = 6
N_VIRT = 112


def setup_inputs(seed: int = 0, part: int = 0) -> dict:
    base_key = jax.random.fold_in(jax.random.key(seed), part)
    key_ints, key_occ, key_vir = jax.random.split(base_key, 3)
    coef_scale = N_BASIS ** -0.5
    ao_ints = jax.random.normal(key_ints, (N_BASIS, N_BASIS, N_BASIS, N_BASIS), jnp.float32).astype(jnp.bfloat16)
    c_occ = (jax.random.normal(key_occ, (N_BASIS, N_OCC), jnp.float32) * coef_scale).astype(jnp.bfloat16)
    c_vir = (jax.random.normal(key_vir, (N_BASIS, N_VIRT), jnp.float32) * coef_scale).astype(jnp.bfloat16)
    return {'ao_ints': ao_ints, 'c_occ': c_occ, 'c_vir': c_vir}


def reference(ao_ints, c_occ, c_vir):
    occ_f32 = c_occ.astype(jnp.float32)
    vir_f32 = c_vir.astype(jnp.float32)
    n_pairs = c_occ.shape[1] * c_vir.shape[1]

    def first_half(ao_row):
        t_one = jnp.einsum('qrs,rj->qsj', ao_row.astype(jnp.float32), occ_f32).astype(jnp.bfloat16)
        half_ints = jnp.einsum('qsj,sb->qjb', t_one.astype(jnp.float32), vir_f32).astype(jnp.bfloat16)
        return half_ints.reshape(ao_row.shape[0], n_pairs)

    half_all = lax.map(first_half, ao_ints)
    g_mid = jnp.einsum('qa,pqc->apc', vir_f32, half_all.astype(jnp.float32))
    return jnp.einsum('pi,apc->iac', occ_f32, g_mid)
```

```python
import functools

import jax
import jax.numpy as jnp
from jax import lax
from jax.experimental import pallas as pl
from jax.experimental.pallas import tpu as pltpu
from jax.sharding import PartitionSpec as P

MESH = pl.DeviceIdType.MESH
F32 = jnp.float32
BF16 = jnp.bfloat16

N_P = 29
N_Q = 58
HALF = 29
N_R = 116
N_OCC = 6
N_VIR = 112
COLS = 84
ROWS = 88
SLOTS = 4


def kernel(a_ref, cot_ref, cvt_ref, out_ref, abuf, lhs1, w2, cvb, cob, t1, acc,
           rb0, rb1x, rb1y, rb2x, rb2y, a_sem, s0_send, s0_recv,
           x_send, x_recv, y_send, y_recv, x2_send, x2_recv, y2_send, y2_recv):
    y = lax.axis_index("dev2")
    dev = lax.axis_index("dev")
    x = dev // 2
    core = dev % 2
    frag = lax.axis_index("frag")
    partner = (frag, y, 2 * x + 1 - core)
    xnbr = (frag, y, 2 * (1 - x) + core)
    ynbr = (frag, 1 - y, dev)

    barrier = pltpu.get_barrier_semaphore()
    for peer in (partner, xnbr, ynbr):
        pl.semaphore_signal(barrier, inc=1, device_id=peer, device_id_type=MESH)

    def fetch(p, slot):
        return pltpu.make_async_copy(
            a_ref.at[p], abuf.at[slot, :, pl.ds(0, N_R)], a_sem.at[slot])

    for p in range(SLOTS):
        fetch(p, p).start()

    for s in range(SLOTS):
        abuf[s, :, N_R:, :] = jnp.zeros((N_Q, 4, N_R), BF16)
    t1[...] = jnp.zeros_like(t1)
    acc[...] = jnp.zeros_like(acc)
    lhs1[...] = jnp.zeros_like(lhs1)
    w2[...] = jnp.zeros_like(w2)
    cvb[...] = jnp.zeros_like(cvb)

    cot = cot_ref[...].astype(F32)
    rep = jnp.concatenate(
        [jnp.broadcast_to(cot[j:j + 1], (8, N_R)) for j in range(N_OCC)], axis=0)
    sub = lax.broadcasted_iota(jnp.int32, (8 * N_OCC, N_R), 0) % 8
    for m in range(8):
        lhs1[m, :, :N_R] = jnp.where(sub == m, rep, 0.0).astype(BF16)

    cvt = cvt_ref[...].astype(F32)

    def put(xt, b, row, col, k):
        pieces = []
        pos = 0
        for n, lo, kk in zip(row, col, k):
            pieces.append((pos, n, lo, kk))
            pos += n
        for kk in (0, 1):
            parts = []
            for start, n, lo, k2 in pieces:
                parts.append(cvt[lo:lo + n] if k2 == kk else jnp.zeros((n, N_R), F32))
            parts.append(jnp.zeros((ROWS - COLS, N_R), F32))
            w2[xt, pl.ds(b * ROWS, ROWS), kk * 128:kk * 128 + N_R] = (
                jnp.concatenate(parts, axis=0).astype(BF16))

    put(0, 0, (84,), (0,), (0,))
    put(0, 1, (28, 56), (84, 0), (0, 1))
    put(1, 0, (56, 28), (56, 0), (0, 1))
    put(1, 1, (84,), (28,), (1,))

    cv = cvt.T
    for h in range(2):
        lo = h * HALF
        mine = jnp.where(y == 0, cv[lo:lo + HALF], cv[N_Q + lo:N_Q + lo + HALF])
        mine = jnp.concatenate([mine, jnp.zeros((3, N_VIR), F32)], axis=0).astype(BF16)
        for k in range(2):
            cvb[pl.ds(k * 64 + h * 32, 32), k * 128:k * 128 + N_VIR] = mine

    co = cot.T
    for i in range(N_OCC):
        cob[i] = jnp.broadcast_to(co[:, i:i + 1], (N_R, 128))

    def first(slot, par, k):
        sums = []
        for g in range(4):
            total = None
            for m in range(min(8, HALF - 8 * g)):
                q = 8 * g + m
                left = jnp.pad(abuf[slot, q], ((0, 0), (0, 12)))
                right = jnp.pad(abuf[slot, HALF + q], ((0, 0), (0, 12)))
                term = jnp.dot(lhs1[m], jnp.concatenate([left, right], axis=1),
                               preferred_element_type=F32)
                total = term if total is None else total + term
            sums.append(total)
        for gp in range(2):
            for j in range(N_OCC):
                for h in range(2):
                    both = jnp.concatenate(
                        [sums[2 * gp + e][8 * j:8 * j + 8, 128 * h:128 * h + 128] for e in range(2)],
                        axis=0)
                    t1[par, j, pl.ds(k * 64 + h * 32 + gp * 16, 16), :] = both.astype(BF16)

    def rest(par, k, group):
        xt = (x + 1 - k // 2) % 2
        yt = (y + 1 - k % 2) % 2
        j0 = 3 * yt + xt
        both = jnp.concatenate([t1[par, j0], t1[par, j0 + 1]], axis=1)
        half = lax.dot_general(w2[xt], both, (((1,), (1,)), ((), ())),
                               preferred_element_type=F32).astype(BF16)
        for b in range(2):
            rows = half[b * ROWS:(b + 1) * ROWS]
            g = []
            for e in range(2):
                two = jnp.dot(rows[:, 128 * e:128 * e + 128], cvb[...], preferred_element_type=F32)
                g += [two[:, :128], two[:, 128:]]
            for i in range(N_OCC):
                v = acc[k, b, i]
                for e in range(4):
                    p = jnp.maximum(4 * group - 3 + e, 0)
                    v = v + cob[i, pl.ds(dev * N_P + p, 1), :] * g[e]
                acc[k, b, i] = v

    def body(p, carry):
        slot = p % SLOTS
        fetch(p, slot).wait()
        n = p + 3
        first(slot, (n // 4) % 2, n % 4)
        rest((n // 4 + 1) % 2, n % 4, n // 4 - 1)

        @pl.when(p + SLOTS < N_P)
        def _():
            fetch(p + SLOTS, slot).start()
        return carry

    lax.fori_loop(0, N_P, body, 0)

    pl.semaphore_wait(barrier, 3)

    def remote(src, dst, send, recv, peer):
        return pltpu.make_async_remote_copy(
            src_ref=src, dst_ref=dst, send_sem=send, recv_sem=recv,
            device_id=peer, device_id_type=MESH)

    def pair(k):
        return remote(acc.at[k, 1 - core], rb0.at[k], s0_send.at[k], s0_recv.at[k], partner)

    def diag_x(i):
        return remote(acc.at[0, core, i], rb1x.at[0, i], x_send.at[0, i], x_recv.at[0, i], xnbr)

    def diag_y(i):
        return remote(acc.at[0, core, 3 + i], rb1y.at[0, i], y_send.at[0, i], y_recv.at[0, i], ynbr)

    def own_x(i):
        return remote(acc.at[1, core, i], rb1x.at[1, i], x_send.at[1, i], x_recv.at[1, i], xnbr)

    def own_y(i):
        return remote(acc.at[2, core, 3 + i], rb1y.at[1, i], y_send.at[1, i], y_recv.at[1, i], ynbr)

    def last_y(i):
        return remote(acc.at[2, core, i], rb2y.at[i], y2_send.at[i], y2_recv.at[i], ynbr)

    def last_x(i):
        return remote(acc.at[1, core, 3 + i], rb2x.at[i], x2_send.at[i], x2_recv.at[i], xnbr)

    def fold(k):
        pair(k).wait_recv()
        acc[k, core] = acc[k, core] + rb0[k]

    rest(1, 0, 7)
    pair(0).start()
    rest(1, 1, 7)
    pair(1).start()
    fold(0)
    for i in range(3):
        diag_x(i).start()
        diag_y(i).start()
    rest(1, 2, 7)
    pair(2).start()
    fold(1)
    for i in range(3):
        own_x(i).start()
    rest(1, 3, 7)
    pair(3).start()
    fold(2)
    for i in range(3):
        own_y(i).start()
    fold(3)
    for i in range(3):
        diag_x(i).wait_recv()
        acc[2, core, i] = acc[2, core, i] + rb1x[0, i]
        last_y(i).start()
        diag_y(i).wait_recv()
        acc[1, core, 3 + i] = acc[1, core, 3 + i] + rb1y[0, i]
        last_x(i).start()
    for i in range(3):
        own_x(i).wait_recv()
        acc[3, core, i] = acc[3, core, i] + rb1x[1, i]
        own_y(i).wait_recv()
        acc[3, core, 3 + i] = acc[3, core, 3 + i] + rb1y[1, i]
    for i in range(3):
        last_y(i).wait_recv()
        out_ref[i] = (acc[3, core, i] + rb2y[i])[:COLS, :N_VIR]
        last_x(i).wait_recv()
        out_ref[3 + i] = (acc[3, core, 3 + i] + rb2x[i])[:COLS, :N_VIR]
    for k in range(4):
        pair(k).wait_send()
    for i in range(3):
        for copy in (diag_x(i), diag_y(i), own_x(i), own_y(i), last_x(i), last_y(i)):
            copy.wait_send()


def solution(mesh):
    def local_program(ints_blk, c_occ, c_vir):
        dma = pltpu.SemaphoreType.DMA
        block = (ROWS, 128)
        out = pl.pallas_call(
            kernel,
            out_shape=jax.ShapeDtypeStruct((N_OCC, COLS, N_VIR), F32),
            in_specs=[pl.BlockSpec(memory_space=pl.ANY),
                      pl.BlockSpec(memory_space=pltpu.VMEM),
                      pl.BlockSpec(memory_space=pltpu.VMEM)],
            out_specs=pl.BlockSpec(memory_space=pltpu.VMEM),
            scratch_shapes=[
                pltpu.VMEM((SLOTS, N_Q, 120, N_R), BF16),
                pltpu.VMEM((8, 8 * N_OCC, 120), BF16),
                pltpu.VMEM((2, 2 * ROWS, 256), BF16),
                pltpu.VMEM((128, 256), BF16),
                pltpu.VMEM((N_OCC, N_R, 128), F32),
                pltpu.VMEM((2, N_OCC, 256, 128), BF16),
                pltpu.VMEM((4, 2, N_OCC) + block, F32),
                pltpu.VMEM((4, N_OCC) + block, F32),
                pltpu.VMEM((2, 3) + block, F32),
                pltpu.VMEM((2, 3) + block, F32),
                pltpu.VMEM((3,) + block, F32),
                pltpu.VMEM((3,) + block, F32),
                dma((SLOTS,)), dma((4,)), dma((4,)),
                dma((2, 3)), dma((2, 3)), dma((2, 3)), dma((2, 3)),
                dma((3,)), dma((3,)), dma((3,)), dma((3,)),
            ],
            compiler_params=pltpu.CompilerParams(
                collective_id=0, has_side_effects=True,
                vmem_limit_bytes=60 * 1024 * 1024),
        )(ints_blk, c_occ.T, c_vir.T)
        return jnp.transpose(out, (0, 2, 1))

    return jax.shard_map(
        local_program,
        mesh=mesh,
        in_specs=(P(('frag', 'dev'), 'dev2', None, None), P('frag', None), P('frag', None)),
        out_specs=P(None, None, ('frag', 'dev2', 'dev')),
        check_vma=False,
    )
```

```python
import functools

import jax
import jax.numpy as jnp
from jax import lax
from jax.experimental import pallas as pl
from jax.experimental.pallas import tpu as pltpu
from jax.sharding import PartitionSpec as P

MESH = pl.DeviceIdType.MESH
F32 = jnp.float32
BF16 = jnp.bfloat16

N_P = 29
N_Q = 58
HALF = 29
N_R = 116
N_OCC = 6
N_VIR = 112
COLS = 84
ROWS = 88
SLOTS = 6


def kernel(a_ref, cot_ref, cvt_ref, out_ref, abuf, lhs1, w2, cvb, cob, t1, ht, acc,
           rb0, rb1x, rb1y, rb2x, rb2y, a_sem, s0_send, s0_recv,
           x_send, x_recv, y_send, y_recv, x2_send, x2_recv, y2_send, y2_recv):
    y = lax.axis_index("dev2")
    dev = lax.axis_index("dev")
    x = dev // 2
    core = dev % 2
    frag = lax.axis_index("frag")
    partner = (frag, y, 2 * x + 1 - core)
    xnbr = (frag, y, 2 * (1 - x) + core)
    ynbr = (frag, 1 - y, dev)

    barrier = pltpu.get_barrier_semaphore()
    for peer in (partner, xnbr, ynbr):
        pl.semaphore_signal(barrier, inc=1, device_id=peer, device_id_type=MESH)

    def fetch(p, slot):
        return pltpu.make_async_copy(
            a_ref.at[p], abuf.at[slot, :, pl.ds(0, N_R)], a_sem.at[slot])

    for p in range(SLOTS):
        fetch(p, p).start()

    for s in range(SLOTS):
        abuf[s, :, N_R:, :] = jnp.zeros((N_Q, 4, N_R), BF16)
    t1[...] = jnp.zeros_like(t1)
    acc[...] = jnp.zeros_like(acc)
    lhs1[...] = jnp.zeros_like(lhs1)
    w2[...] = jnp.zeros_like(w2)
    cvb[...] = jnp.zeros_like(cvb)
    ht[...] = jnp.zeros_like(ht)

    cot = cot_ref[...].astype(F32)
    rep = jnp.concatenate(
        [jnp.broadcast_to(cot[j:j + 1], (8, N_R)) for j in range(N_OCC)], axis=0)
    sub = lax.broadcasted_iota(jnp.int32, (8 * N_OCC, N_R), 0) % 8
    for m in range(8):
        lhs1[m, :, :N_R] = jnp.where(sub == m, rep, 0.0).astype(BF16)

    cvt = cvt_ref[...].astype(F32)

    def put(xt, b, row, col, k):
        pieces = []
        pos = 0
        for n, lo, kk in zip(row, col, k):
            pieces.append((pos, n, lo, kk))
            pos += n
        for kk in (0, 1):
            parts = []
            for start, n, lo, k2 in pieces:
                parts.append(cvt[lo:lo + n] if k2 == kk else jnp.zeros((n, N_R), F32))
            parts.append(jnp.zeros((ROWS - COLS, N_R), F32))
            w2[xt, pl.ds(b * ROWS, ROWS), kk * 128:kk * 128 + N_R] = (
                jnp.concatenate(parts, axis=0).astype(BF16))

    put(0, 0, (84,), (0,), (0,))
    put(0, 1, (28, 56), (84, 0), (0, 1))
    put(1, 0, (56, 28), (56, 0), (0, 1))
    put(1, 1, (84,), (28,), (1,))

    cv = cvt.T
    for h in range(2):
        lo = h * HALF
        mine = jnp.where(y == 0, cv[lo:lo + HALF], cv[N_Q + lo:N_Q + lo + HALF])
        mine = jnp.concatenate([mine, jnp.zeros((3, N_VIR), F32)], axis=0).astype(BF16)
        for k in range(2):
            cvb[pl.ds(k * 64 + h * 32, 32), k * 128:k * 128 + N_VIR] = mine

    co = cot.T
    for i in range(N_OCC):
        cob[i] = jnp.broadcast_to(co[:, i:i + 1], (N_R, 128))

    def first(slot, par, k):
        sums = []
        for g in range(4):
            total = None
            for m in range(min(8, HALF - 8 * g)):
                q = 8 * g + m
                left = jnp.pad(abuf[slot, q], ((0, 0), (0, 12)))
                right = jnp.pad(abuf[slot, HALF + q], ((0, 0), (0, 12)))
                term = jnp.dot(lhs1[m], jnp.concatenate([left, right], axis=1),
                               preferred_element_type=F32)
                total = term if total is None else total + term
            sums.append(total)
        for gp in range(2):
            for j in range(N_OCC):
                for h in range(2):
                    both = jnp.concatenate(
                        [sums[2 * gp + e][8 * j:8 * j + 8, 128 * h:128 * h + 128] for e in range(2)],
                        axis=0)
                    t1[par, j, pl.ds(k * 64 + h * 32 + gp * 16, 16), :] = both.astype(BF16)

    def place(k):
        return (x + 1 - k // 2) % 2, (y + 1 - k % 2) % 2

    def second(par, k):
        xt, yt = place(k)
        j0 = 3 * yt + xt
        both = jnp.concatenate([t1[par, j0], t1[par, j0 + 1]], axis=1)
        return lax.dot_general(w2[xt], both, (((1,), (1,)), ((), ())),
                               preferred_element_type=F32).astype(BF16)

    def third(half, k, group):
        two = jnp.dot(jnp.concatenate([half[:, :128], half[:, 128:]], axis=0), cvb[...],
                      preferred_element_type=F32)
        scale = []
        for e in range(4):
            p = dev * N_P + jnp.maximum(4 * group - 3 + e, 0)
            scale.append([jnp.broadcast_to(cob[i, pl.ds(p, 1), :], (8, 128)) for i in range(N_OCC)])
        for b in range(2):
            for r in range(ROWS // 8):
                at = b * ROWS + 8 * r
                g = [two[at + 2 * ROWS * (e // 2):at + 2 * ROWS * (e // 2) + 8,
                         128 * (e % 2):128 * (e % 2) + 128] for e in range(4)]
                for i in range(N_OCC):
                    v = acc[k, b, i, 8 * r:8 * r + 8]
                    for e in range(4):
                        v = v + scale[e][i] * g[e]
                    acc[k, b, i, 8 * r:8 * r + 8] = v

    def refill(p):
        @pl.when(p + SLOTS < N_P)
        def _():
            fetch(p + SLOTS, p % SLOTS).start()

    fetch(0, 0).wait()
    first(0, 0, 3)
    refill(0)

    def body(u, carry):
        p = 1 + 2 * u
        group, k = 1 + u // 2, 2 * (u % 2)
        before = jnp.maximum(u - 1, 0) // 2
        fetch(p, p % SLOTS).wait()
        fetch(p + 1, (p + 1) % SLOTS).wait()
        third(ht[0], 2 - k, before)
        third(ht[1], 3 - k, before)
        left = second((group + 1) % 2, k)
        right = second((group + 1) % 2, k + 1)
        first(p % SLOTS, group % 2, k)
        first((p + 1) % SLOTS, group % 2, k + 1)
        ht[0] = left
        ht[1] = right
        refill(p)
        refill(p + 1)
        return carry

    lax.fori_loop(0, 13, body, 0)
    third(ht[0], 0, 6)
    third(ht[1], 1, 6)
    for k in (2, 3):
        third(second(0, k), k, 6)
    fetch(27, 27 % SLOTS).wait()
    first(27 % SLOTS, 1, 2)
    fetch(28, 28 % SLOTS).wait()
    first(28 % SLOTS, 1, 3)

    pl.semaphore_wait(barrier, 3)

    def remote(src, dst, send, recv, peer):
        return pltpu.make_async_remote_copy(
            src_ref=src, dst_ref=dst, send_sem=send, recv_sem=recv,
            device_id=peer, device_id_type=MESH)

    def pair(k):
        return remote(acc.at[k, 1 - core], rb0.at[k], s0_send.at[k], s0_recv.at[k], partner)

    def diag_x(i):
        return remote(acc.at[0, core, i], rb1x.at[0, i], x_send.at[0, i], x_recv.at[0, i], xnbr)

    def diag_y(i):
        return remote(acc.at[0, core, 3 + i], rb1y.at[0, i], y_send.at[0, i], y_recv.at[0, i], ynbr)

    def own_x(i):
        return remote(acc.at[1, core, i], rb1x.at[1, i], x_send.at[1, i], x_recv.at[1, i], xnbr)

    def own_y(i):
        return remote(acc.at[2, core, 3 + i], rb1y.at[1, i], y_send.at[1, i], y_recv.at[1, i], ynbr)

    def last_y(i):
        return remote(acc.at[2, core, i], rb2y.at[i], y2_send.at[i], y2_recv.at[i], ynbr)

    def last_x(i):
        return remote(acc.at[1, core, 3 + i], rb2x.at[i], x2_send.at[i], x2_recv.at[i], xnbr)

    def fold(k):
        pair(k).wait_recv()
        acc[k, core] = acc[k, core] + rb0[k]

    h0 = second(1, 0)
    h1 = second(1, 1)
    third(h0, 0, 7)
    pair(0).start()
    h2 = second(1, 2)
    third(h1, 1, 7)
    pair(1).start()
    h3 = second(1, 3)
    third(h2, 2, 7)
    pair(2).start()
    fold(0)
    for i in range(3):
        diag_x(i).start()
        diag_y(i).start()
    third(h3, 3, 7)
    pair(3).start()
    fold(1)
    for i in range(3):
        own_x(i).start()
    fold(2)
    for i in range(3):
        own_y(i).start()
    fold(3)
    for i in range(3):
        diag_x(i).wait_recv()
        acc[2, core, i] = acc[2, core, i] + rb1x[0, i]
        last_y(i).start()
        diag_y(i).wait_recv()
        acc[1, core, 3 + i] = acc[1, core, 3 + i] + rb1y[0, i]
        last_x(i).start()
    for i in range(3):
        own_x(i).wait_recv()
        acc[3, core, i] = acc[3, core, i] + rb1x[1, i]
        own_y(i).wait_recv()
        acc[3, core, 3 + i] = acc[3, core, 3 + i] + rb1y[1, i]
    for i in range(3):
        last_y(i).wait_recv()
        out_ref[i] = (acc[3, core, i] + rb2y[i])[:COLS, :N_VIR]
        last_x(i).wait_recv()
        out_ref[3 + i] = (acc[3, core, 3 + i] + rb2x[i])[:COLS, :N_VIR]
    for k in range(4):
        pair(k).wait_send()
    for i in range(3):
        for copy in (diag_x(i), diag_y(i), own_x(i), own_y(i), last_x(i), last_y(i)):
            copy.wait_send()


def solution(mesh):
    def local_program(ints_blk, c_occ, c_vir):
        dma = pltpu.SemaphoreType.DMA
        block = (ROWS, 128)
        out = pl.pallas_call(
            kernel,
            out_shape=jax.ShapeDtypeStruct((N_OCC, COLS, N_VIR), F32),
            in_specs=[pl.BlockSpec(memory_space=pl.ANY),
                      pl.BlockSpec(memory_space=pltpu.VMEM),
                      pl.BlockSpec(memory_space=pltpu.VMEM)],
            out_specs=pl.BlockSpec(memory_space=pltpu.VMEM),
            scratch_shapes=[
                pltpu.VMEM((SLOTS, N_Q, 120, N_R), BF16),
                pltpu.VMEM((8, 8 * N_OCC, 120), BF16),
                pltpu.VMEM((2, 2 * ROWS, 256), BF16),
                pltpu.VMEM((128, 256), BF16),
                pltpu.VMEM((N_OCC, N_R, 128), F32),
                pltpu.VMEM((2, N_OCC, 256, 128), BF16),
                pltpu.VMEM((2, 2 * ROWS, 256), BF16),
                pltpu.VMEM((4, 2, N_OCC) + block, F32),
                pltpu.VMEM((4, N_OCC) + block, F32),
                pltpu.VMEM((2, 3) + block, F32),
                pltpu.VMEM((2, 3) + block, F32),
                pltpu.VMEM((3,) + block, F32),
                pltpu.VMEM((3,) + block, F32),
                dma((SLOTS,)), dma((4,)), dma((4,)),
                dma((2, 3)), dma((2, 3)), dma((2, 3)), dma((2, 3)),
                dma((3,)), dma((3,)), dma((3,)), dma((3,)),
            ],
            compiler_params=pltpu.CompilerParams(
                collective_id=0, has_side_effects=True,
                vmem_limit_bytes=28 * 1024 * 1024),
        )(ints_blk, c_occ.T, c_vir.T)
        return jnp.transpose(out, (0, 2, 1))

    return jax.shard_map(
        local_program,
        mesh=mesh,
        in_specs=(P(('frag', 'dev'), 'dev2', None, None), P('frag', None), P('frag', None)),
        out_specs=P(None, None, ('frag', 'dev2', 'dev')),
        check_vma=False,
    )
```

```python
import jax
import jax.numpy as jnp
from jax import lax
from jax.experimental import pallas as pl
from jax.experimental.pallas import tpu as pltpu
from jax.sharding import PartitionSpec as P

MESH = pl.DeviceIdType.MESH
F32 = jnp.float32
BF16 = jnp.bfloat16

N_P = 29
N_Q = 58
HALF = 29
N_R = 116
N_OCC = 6
N_VIR = 112
COLS = 84
XC = 40
YC = 44
YR = 48
SLOTS = 6
PAIRS = 15
LAG = 5


def kernel(a_ref, cot_ref, cvt_ref, out_ref, cot_v, cvt_v, abuf, lhs1, w2, cvb, cob, t1,
           lx, ly, xs, ys, px, py, xr, yr, acc_x, acc_y, vx, vy,
           a_sem, c_sem, send, recv, v_send, v_recv):
    frag = lax.axis_index("frag")
    y = lax.axis_index("dev2")
    dev = lax.axis_index("dev")
    x = dev // 2
    core = dev % 2
    partner = (frag, y, 2 * x + 1 - core)
    xnbr = [(frag, y, 2 * (1 - x) + b) for b in range(2)]
    ynbr = [(frag, 1 - y, 2 * x + b) for b in range(2)]

    small = [pltpu.make_async_copy(cot_ref, cot_v, c_sem.at[0]),
             pltpu.make_async_copy(cvt_ref, cvt_v, c_sem.at[1])]
    for copy in small:
        copy.start()

    def fetch(p, slot):
        return pltpu.make_async_copy(
            a_ref.at[p], abuf.at[slot, :, pl.ds(0, N_R)], a_sem.at[slot])

    for p in range(SLOTS):
        fetch(p, p).start()

    rest = jnp.zeros((PAIRS, 2, 2, YR - YC, 128), BF16)
    yr[:, :, :, YC:, :] = rest
    py[:, :, YC:, :] = rest[:, 0]

    barrier = pltpu.get_barrier_semaphore()
    for peer in [partner] + xnbr + ynbr:
        pl.semaphore_signal(barrier, inc=1, device_id=peer, device_id_type=MESH)

    for s in range(SLOTS):
        abuf[s, :, N_R:, :] = jnp.zeros((N_Q, 4, N_R), BF16)
    acc_x[...] = jnp.zeros_like(acc_x)
    acc_y[...] = jnp.zeros_like(acc_y)
    lhs1[...] = jnp.zeros_like(lhs1)
    w2[...] = jnp.zeros_like(w2)
    cvb[...] = jnp.zeros_like(cvb)
    cob[...] = jnp.zeros_like(cob)
    for copy in small:
        copy.wait()

    cot = cot_v[...].astype(F32)
    rep = jnp.concatenate(
        [jnp.broadcast_to(cot[j:j + 1], (8, N_R)) for j in range(N_OCC)], axis=0)
    sub = lax.broadcasted_iota(jnp.int32, (8 * N_OCC, N_R), 0) % 8
    for m in range(8):
        lhs1[m, :, :N_R] = jnp.where(sub == m, rep, 0.0).astype(BF16)

    cvt = cvt_v[...].astype(F32)

    def put(xt, b, pieces):
        for kk in (0, 1):
            rows = jnp.concatenate(
                [cvt[lo:lo + n] if k == kk else jnp.zeros((n, N_R), F32) for n, lo, k in pieces]
                + [jnp.zeros((YR - YC, N_R), F32)], axis=0).astype(BF16)
            w2[xt, pl.ds(b * XC, XC), kk * 128:kk * 128 + N_R] = rows[:XC]
            w2[xt, pl.ds(2 * XC + b * YR, YR), kk * 128:kk * 128 + N_R] = rows[XC:]

    put(0, 0, [(84, 0, 0)])
    put(0, 1, [(28, 84, 0), (56, 0, 1)])
    put(1, 0, [(56, 56, 0), (28, 0, 1)])
    put(1, 1, [(84, 28, 1)])

    cv = cvt.T
    for side in range(2):
        for h in range(2):
            lo = h * HALF
            low, high = cv[lo:lo + HALF], cv[N_Q + lo:N_Q + lo + HALF]
            part = jnp.where(y == side, low, high)
            part = jnp.concatenate([part, jnp.zeros((3, N_VIR), F32)], axis=0).astype(BF16)
            for k in range(2):
                cvb[pl.ds(side * 128 + k * 64 + h * 32, 32), k * 128:k * 128 + N_VIR] = part

    co = cot.T
    for i in range(N_OCC):
        cob[i, :N_R] = jnp.broadcast_to(co[:, i:i + 1], (N_R, 128))

    def first(slot, par, k):
        sums = []
        for g in range(4):
            total = None
            for m in range(min(8, HALF - 8 * g)):
                q = 8 * g + m
                left = jnp.pad(abuf[slot, q], ((0, 0), (0, 12)))
                right = jnp.pad(abuf[slot, HALF + q], ((0, 0), (0, 12)))
                term = jnp.dot(lhs1[m], jnp.concatenate([left, right], axis=1),
                               preferred_element_type=F32)
                total = term if total is None else total + term
            sums.append(total)
        for gp in range(2):
            for j in range(N_OCC):
                for h in range(2):
                    both = jnp.concatenate(
                        [sums[2 * gp + e][8 * j:8 * j + 8, 128 * h:128 * h + 128] for e in range(2)],
                        axis=0)
                    t1[par, j, k * 64 + h * 32 + gp * 16:k * 64 + h * 32 + gp * 16 + 16, :] = (
                        both.astype(BF16))

    def second(par, u):
        for dx in range(2):
            xt = (x + dx) % 2
            rows = []
            for dy in range(2):
                j0 = 3 * ((y + dy) % 2) + xt
                rows.append(jnp.concatenate([t1[par, j0], t1[par, j0 + 1]], axis=1))
            half = lax.dot_general(w2[xt], jnp.concatenate(rows, axis=0), (((1,), (1,)), ((), ())),
                                   preferred_element_type=F32).astype(BF16)
            for b in range(2):
                for dy in range(2):
                    lane = slice(128 * dy, 128 * dy + 128)
                    (lx, xs)[dx][u, b, dy] = half[b * XC:(b + 1) * XC, lane]
                    (ly, ys)[dy][u, b, dx] = half[2 * XC + b * YR:2 * XC + (b + 1) * YR, lane]

    def remote(src, dst, s, r, peer):
        return pltpu.make_async_remote_copy(
            src_ref=src, dst_ref=dst, send_sem=s, recv_sem=r, device_id=peer, device_id_type=MESH)

    live = pl.ds(0, YC)

    def cross_x(u, b, mark):
        return remote(xs.at[u, b], xr.at[u, core], send.at[u, b], recv.at[u, mark], xnbr[b])

    def cross_y(u, b, mark):
        return remote(ys.at[u, b, :, live], yr.at[u, core, :, live], send.at[u, 2 + b],
                      recv.at[u, 2 + mark], ynbr[b])

    def pair_x(u):
        return remote(lx.at[u, 1 - core], px.at[u], send.at[u, 4], recv.at[u, 4], partner)

    def pair_y(u):
        return remote(ly.at[u, 1 - core, :, live], py.at[u, :, live], send.at[u, 5],
                      recv.at[u, 5], partner)

    def send_pair(u):
        for b in range(2):
            cross_y(u, b, core).start()
            cross_x(u, b, core).start()
        pair_x(u).start()
        pair_y(u).start()

    def arrive(u):
        for b in range(2):
            cross_x(u, b, b).wait_recv()
            cross_y(u, b, b).wait_recv()
        pair_x(u).wait_recv()
        pair_y(u).wait_recv()

    def scales(u, source):
        p = source * N_P + 2 * u
        return [[jnp.broadcast_to(cob[i, pl.ds(p + e, 1), :], (8, 128)) for i in range(N_OCC)]
                for e in range(2)]

    def gather_x(acc, d, tiles, g, scale):
        for r in range(tiles):
            for i in range(N_OCC):
                v = acc[d, i, 8 * r:8 * r + 8]
                for rows, sc in zip(g, scale):
                    for e in range(2):
                        v = v + sc[e][i] * rows[8 * r:8 * r + 8, 128 * e:128 * e + 128]
                acc[d, i, 8 * r:8 * r + 8] = v

    def third(u, order=(0, 1)):
        flat = [lx[u, core], px[u], xr[u, 0], xr[u, 1]]
        from_x = [dev, 2 * x + 1 - core, 2 * (1 - x), 2 * (1 - x) + 1]
        ys_in = [jnp.concatenate([ly[u, core], yr[u, core]], axis=2),
                 jnp.concatenate([py[u], yr[u, 1 - core]], axis=2)]
        from_y = from_x[:2]
        gx = jnp.dot(jnp.concatenate([f[d] for d in order for f in flat], axis=0), cvb[:128],
                     preferred_element_type=F32)
        gy = jnp.dot(jnp.concatenate([f[d] for d in order for f in ys_in], axis=0), cvb[...],
                     preferred_element_type=F32)
        for n, d in enumerate(order):
            for s in range(0, 4, 2):
                at = (4 * n + s) * XC
                gather_x(acc_x, d, XC // 8, [gx[at:at + XC], gx[at + XC:at + 2 * XC]],
                         [scales(u, from_x[s]), scales(u, from_x[s + 1])])
            at = 2 * n * YR
            gather_x(acc_y, d, YR // 8, [gy[at:at + YR], gy[at + YR:at + 2 * YR]],
                     [scales(u, from_y[0]), scales(u, from_y[1])])

    def refill(p):
        @pl.when(p + SLOTS < N_P)
        def _():
            fetch(p + SLOTS, p % SLOTS).start()

    def stream(u):
        p = 2 * u
        fetch(p, p % SLOTS).wait()
        fetch(p + 1, (p + 1) % SLOTS).wait()

    def trip(u):
        p = 2 * u
        first(p % SLOTS, u % 2, 0)
        first((p + 1) % SLOTS, u % 2, 1)

    def after(u):
        refill(2 * u)
        refill(2 * u + 1)

    stream(0)
    trip(0)
    after(0)
    pl.semaphore_wait(barrier, 5)

    def early(u, carry):
        stream(u)
        second((u + 1) % 2, u - 1)
        trip(u)
        send_pair(u - 1)
        after(u)
        return carry

    def late(u, carry):
        stream(u)
        arrive(u - LAG)
        third(u - LAG)
        second((u + 1) % 2, u - 1)
        trip(u)
        send_pair(u - 1)
        after(u)
        return carry

    lax.fori_loop(1, LAG, early, 0)
    lax.fori_loop(LAG, PAIRS - 1, late, 0)

    last = PAIRS - 1
    second(1, last - 1)
    send_pair(last - 1)
    t1[0, :, 64:, :] = jnp.zeros((N_OCC, 64, 128), BF16)
    fetch(N_P - 1, (N_P - 1) % SLOTS).wait()
    first((N_P - 1) % SLOTS, 0, 0)
    second(0, last)
    send_pair(last)

    def drain(u, carry):
        arrive(u)
        third(u)
        return carry

    lax.fori_loop(last - LAG, last, drain, 0)
    arrive(last)
    third(last, (1, 0))

    def v_y(i):
        return remote(acc_x.at[1, i], vy.at[i], v_send.at[0, i], v_recv.at[0, i], (frag, 1 - y, dev))

    def v_x(i):
        return remote(acc_y.at[1, i, live], vx.at[i, live], v_send.at[1, i], v_recv.at[1, i],
                      (frag, y, 2 * (1 - x) + core))

    for i in range(N_OCC):
        v_y(i).start()
        v_x(i).start()
    for i in range(N_OCC):
        v_y(i).wait_recv()
        out_ref[i, :XC] = (acc_x[0, i] + vy[i])[:, :N_VIR]
        v_x(i).wait_recv()
        out_ref[i, XC:] = (acc_y[0, i, :YC] + vx[i, :YC])[:, :N_VIR]
    for i in range(N_OCC):
        v_y(i).wait_send()
        v_x(i).wait_send()

    def sent(u, carry):
        for b in range(2):
            cross_x(u, b, b).wait_send()
            cross_y(u, b, b).wait_send()
        pair_x(u).wait_send()
        pair_y(u).wait_send()
        return carry

    lax.fori_loop(0, PAIRS, sent, 0)


def solution(mesh):
    def local_program(ints_blk, c_occ, c_vir):
        dma = pltpu.SemaphoreType.DMA
        xb, yb = (2, XC, 128), (2, YR, 128)
        out = pl.pallas_call(
            kernel,
            out_shape=jax.ShapeDtypeStruct((N_OCC, COLS, N_VIR), F32),
            in_specs=[pl.BlockSpec(memory_space=pl.ANY)] * 3,
            out_specs=pl.BlockSpec(memory_space=pltpu.VMEM),
            scratch_shapes=[
                pltpu.VMEM((N_OCC, N_R), BF16),
                pltpu.VMEM((N_VIR, N_R), BF16),
                pltpu.VMEM((SLOTS, N_Q, 120, N_R), BF16),
                pltpu.VMEM((8, 8 * N_OCC, 120), BF16),
                pltpu.VMEM((2, 2 * (XC + YR), 256), BF16),
                pltpu.VMEM((256, 256), BF16),
                pltpu.VMEM((N_OCC, 120, 128), F32),
                pltpu.VMEM((2, N_OCC, 128, 128), BF16),
                pltpu.VMEM((PAIRS, 2) + xb, BF16),
                pltpu.VMEM((PAIRS, 2) + yb, BF16),
                pltpu.VMEM((PAIRS, 2) + xb, BF16),
                pltpu.VMEM((PAIRS, 2) + yb, BF16),
                pltpu.VMEM((PAIRS,) + xb, BF16),
                pltpu.VMEM((PAIRS,) + yb, BF16),
                pltpu.VMEM((PAIRS, 2) + xb, BF16),
                pltpu.VMEM((PAIRS, 2) + yb, BF16),
                pltpu.VMEM((2, N_OCC, XC, 128), F32),
                pltpu.VMEM((2, N_OCC, YR, 128), F32),
                pltpu.VMEM((N_OCC, YR, 128), F32),
                pltpu.VMEM((N_OCC, XC, 128), F32),
                dma((SLOTS,)), dma((2,)), dma((PAIRS, 6)), dma((PAIRS, 6)),
                dma((2, N_OCC)), dma((2, N_OCC)),
            ],
            compiler_params=pltpu.CompilerParams(
                collective_id=0, has_side_effects=True,
                vmem_limit_bytes=36 * 1024 * 1024),
        )(ints_blk, c_occ.T, c_vir.T)
        return jnp.transpose(out, (0, 2, 1))

    return jax.shard_map(
        local_program,
        mesh=mesh,
        in_specs=(P(('frag', 'dev'), 'dev2', None, None), P('frag', None), P('frag', None)),
        out_specs=P(None, None, ('frag', 'dev2', 'dev')),
        check_vma=False,
    )
```

```python
import jax
import jax.numpy as jnp
from jax import lax
from jax.experimental import pallas as pl
from jax.experimental.pallas import tpu as pltpu
from jax.sharding import PartitionSpec as P

MESH = pl.DeviceIdType.MESH
F32 = jnp.float32
BF16 = jnp.bfloat16

N_P = 29
N_Q = 58
HALF = 29
N_R = 116
N_OCC = 6
N_VIR = 112
COLS = 84
XC = 40
YC = 44
YR = 48
SLOTS = 6
PAIRS = 15
LAG = 7


def kernel(a_ref, cot_ref, cvt_ref, out_ref, cot_v, cvt_v, abuf, lhs1, w2, cvb, cob, t1,
           lx, ly, xs, ys, px, py, xr, yr, acc_x, acc_y, vx, vy,
           a_sem, c_sem, send, recv, v_send, v_recv):
    frag = lax.axis_index("frag")
    y = lax.axis_index("dev2")
    dev = lax.axis_index("dev")
    x = dev // 2
    core = dev % 2
    partner = (frag, y, 2 * x + 1 - core)
    xnbr = [(frag, y, 2 * (1 - x) + b) for b in range(2)]
    ynbr = [(frag, 1 - y, 2 * x + b) for b in range(2)]

    small = [pltpu.make_async_copy(cot_ref, cot_v, c_sem.at[0]),
             pltpu.make_async_copy(cvt_ref, cvt_v, c_sem.at[1])]
    for copy in small:
        copy.start()

    def fetch(p, slot):
        return pltpu.make_async_copy(
            a_ref.at[p], abuf.at[slot, :, pl.ds(0, N_R)], a_sem.at[slot])

    for p in range(SLOTS):
        fetch(p, p).start()

    rest = jnp.zeros((PAIRS, 2, 2, YR - YC, 128), BF16)
    yr[:, :, :, YC:, :] = rest
    py[:, :, YC:, :] = rest[:, 0]

    barrier = pltpu.get_barrier_semaphore()
    for peer in [partner] + xnbr + ynbr:
        pl.semaphore_signal(barrier, inc=1, device_id=peer, device_id_type=MESH)

    for s in range(SLOTS):
        abuf[s, :, N_R:, :] = jnp.zeros((N_Q, 4, N_R), BF16)
    acc_x[...] = jnp.zeros_like(acc_x)
    acc_y[...] = jnp.zeros_like(acc_y)
    lhs1[...] = jnp.zeros_like(lhs1)
    w2[...] = jnp.zeros_like(w2)
    cvb[...] = jnp.zeros_like(cvb)
    cob[...] = jnp.zeros_like(cob)
    for copy in small:
        copy.wait()

    cot = cot_v[...].astype(F32)
    rep = jnp.concatenate(
        [jnp.broadcast_to(cot[j:j + 1], (8, N_R)) for j in range(N_OCC)], axis=0)
    sub = lax.broadcasted_iota(jnp.int32, (8 * N_OCC, N_R), 0) % 8
    for m in range(8):
        lhs1[m, :, :N_R] = jnp.where(sub == m, rep, 0.0).astype(BF16)

    cvt = cvt_v[...].astype(F32)

    def put(xt, b, pieces):
        for kk in (0, 1):
            rows = jnp.concatenate(
                [cvt[lo:lo + n] if k == kk else jnp.zeros((n, N_R), F32) for n, lo, k in pieces]
                + [jnp.zeros((YR - YC, N_R), F32)], axis=0).astype(BF16)
            w2[xt, pl.ds(b * XC, XC), kk * 128:kk * 128 + N_R] = rows[:XC]
            w2[xt, pl.ds(2 * XC + b * YR, YR), kk * 128:kk * 128 + N_R] = rows[XC:]

    put(0, 0, [(84, 0, 0)])
    put(0, 1, [(28, 84, 0), (56, 0, 1)])
    put(1, 0, [(56, 56, 0), (28, 0, 1)])
    put(1, 1, [(84, 28, 1)])

    cv = cvt.T
    for side in range(2):
        for h in range(2):
            lo = h * HALF
            low, high = cv[lo:lo + HALF], cv[N_Q + lo:N_Q + lo + HALF]
            part = jnp.where(y == side, low, high)
            part = jnp.concatenate([part, jnp.zeros((3, N_VIR), F32)], axis=0).astype(BF16)
            for k in range(2):
                cvb[pl.ds(side * 128 + k * 64 + h * 32, 32), k * 128:k * 128 + N_VIR] = part

    co = cot.T
    for i in range(N_OCC):
        cob[i, :N_R] = jnp.broadcast_to(co[:, i:i + 1], (N_R, 128))

    def first(slot, par, k):
        sums = []
        for g in range(4):
            total = None
            for m in range(min(8, HALF - 8 * g)):
                q = 8 * g + m
                left = jnp.pad(abuf[slot, q], ((0, 0), (0, 12)))
                right = jnp.pad(abuf[slot, HALF + q], ((0, 0), (0, 12)))
                term = jnp.dot(lhs1[m], jnp.concatenate([left, right], axis=1),
                               preferred_element_type=F32)
                total = term if total is None else total + term
            sums.append(total)
        for gp in range(2):
            for j in range(N_OCC):
                for h in range(2):
                    both = jnp.concatenate(
                        [sums[2 * gp + e][8 * j:8 * j + 8, 128 * h:128 * h + 128] for e in range(2)],
                        axis=0)
                    t1[par, j, k * 64 + h * 32 + gp * 16:k * 64 + h * 32 + gp * 16 + 16, :] = (
                        both.astype(BF16))

    def second(par, u):
        for dx in range(2):
            xt = (x + dx) % 2
            rows = []
            for dy in range(2):
                j0 = 3 * ((y + dy) % 2) + xt
                rows.append(jnp.concatenate([t1[par, j0], t1[par, j0 + 1]], axis=1))
            half = lax.dot_general(w2[xt], jnp.concatenate(rows, axis=0), (((1,), (1,)), ((), ())),
                                   preferred_element_type=F32).astype(BF16)
            for b in range(2):
                for dy in range(2):
                    lane = slice(128 * dy, 128 * dy + 128)
                    (lx, xs)[dx][u, b, dy] = half[b * XC:(b + 1) * XC, lane]
                    (ly, ys)[dy][u, b, dx] = half[2 * XC + b * YR:2 * XC + (b + 1) * YR, lane]

    def remote(src, dst, s, r, peer):
        return pltpu.make_async_remote_copy(
            src_ref=src, dst_ref=dst, send_sem=s, recv_sem=r, device_id=peer, device_id_type=MESH)

    live = pl.ds(0, YC)

    def cross_x(u, b, mark):
        return remote(xs.at[u, b], xr.at[u, core], send.at[u, b], recv.at[u, mark], xnbr[b])

    def cross_y(u, b, mark):
        return remote(ys.at[u, b, :, live], yr.at[u, core, :, live], send.at[u, 2 + b],
                      recv.at[u, 2 + mark], ynbr[b])

    def pair_x(u):
        return remote(lx.at[u, 1 - core], px.at[u], send.at[u, 4], recv.at[u, 4], partner)

    def pair_y(u):
        return remote(ly.at[u, 1 - core, :, live], py.at[u, :, live], send.at[u, 5],
                      recv.at[u, 5], partner)

    def send_pair(u):
        for b in range(2):
            cross_y(u, b, core).start()
            cross_x(u, b, core).start()
        pair_x(u).start()
        pair_y(u).start()

    def arrive(u):
        for b in range(2):
            cross_x(u, b, b).wait_recv()
            cross_y(u, b, b).wait_recv()
        pair_x(u).wait_recv()
        pair_y(u).wait_recv()

    def scales(u, source):
        p = source * N_P + 2 * u
        return [[jnp.broadcast_to(cob[i, pl.ds(p + e, 1), :], (8, 128)) for i in range(N_OCC)]
                for e in range(2)]

    def gather_x(acc, d, tiles, g, scale):
        for r in range(tiles):
            for i in range(N_OCC):
                v = acc[d, i, 8 * r:8 * r + 8]
                for rows, sc in zip(g, scale):
                    for e in range(2):
                        v = v + sc[e][i] * rows[8 * r:8 * r + 8, 128 * e:128 * e + 128]
                acc[d, i, 8 * r:8 * r + 8] = v

    def third(u, order=(0, 1)):
        flat = [lx[u, core], px[u], xr[u, 0], xr[u, 1]]
        from_x = [dev, 2 * x + 1 - core, 2 * (1 - x), 2 * (1 - x) + 1]
        ys_in = [jnp.concatenate([ly[u, core], yr[u, core]], axis=2),
                 jnp.concatenate([py[u], yr[u, 1 - core]], axis=2)]
        from_y = from_x[:2]
        gx = jnp.dot(jnp.concatenate([f[d] for d in order for f in flat], axis=0), cvb[:128],
                     preferred_element_type=F32)
        gy = jnp.dot(jnp.concatenate([f[d] for d in order for f in ys_in], axis=0), cvb[...],
                     preferred_element_type=F32)
        for n, d in enumerate(order):
            for s in range(0, 4, 2):
                at = (4 * n + s) * XC
                gather_x(acc_x, d, XC // 8, [gx[at:at + XC], gx[at + XC:at + 2 * XC]],
                         [scales(u, from_x[s]), scales(u, from_x[s + 1])])
            at = 2 * n * YR
            gather_x(acc_y, d, YR // 8, [gy[at:at + YR], gy[at + YR:at + 2 * YR]],
                     [scales(u, from_y[0]), scales(u, from_y[1])])

    def refill(p):
        @pl.when(p + SLOTS < N_P)
        def _():
            fetch(p + SLOTS, p % SLOTS).start()

    def stream(u):
        p = 2 * u
        fetch(p, p % SLOTS).wait()
        fetch(p + 1, (p + 1) % SLOTS).wait()

    def trip(u):
        p = 2 * u
        first(p % SLOTS, u % 2, 0)
        first((p + 1) % SLOTS, u % 2, 1)

    def after(u):
        refill(2 * u)
        refill(2 * u + 1)

    stream(0)
    trip(0)
    after(0)
    pl.semaphore_wait(barrier, 5)

    def early(u, carry):
        stream(u)
        second((u + 1) % 2, u - 1)
        trip(u)
        send_pair(u - 1)
        after(u)
        return carry

    def late(u, carry):
        stream(u)
        arrive(u - LAG)
        third(u - LAG)
        second((u + 1) % 2, u - 1)
        trip(u)
        send_pair(u - 1)
        after(u)
        return carry

    lax.fori_loop(1, LAG, early, 0)
    lax.fori_loop(LAG, PAIRS - 1, late, 0)

    last = PAIRS - 1
    second(1, last - 1)
    send_pair(last - 1)
    t1[0, :, 64:, :] = jnp.zeros((N_OCC, 64, 128), BF16)
    fetch(N_P - 1, (N_P - 1) % SLOTS).wait()
    first((N_P - 1) % SLOTS, 0, 0)
    second(0, last)
    send_pair(last)

    def drain(u, carry):
        arrive(u)
        third(u)
        return carry

    lax.fori_loop(last - LAG, last, drain, 0)
    arrive(last)
    third(last, (1, 0))

    def v_y(i):
        return remote(acc_x.at[1, i], vy.at[i], v_send.at[0, i], v_recv.at[0, i], (frag, 1 - y, dev))

    def v_x(i):
        return remote(acc_y.at[1, i, live], vx.at[i, live], v_send.at[1, i], v_recv.at[1, i],
                      (frag, y, 2 * (1 - x) + core))

    for i in range(N_OCC):
        v_y(i).start()
        v_x(i).start()
    for i in range(N_OCC):
        v_y(i).wait_recv()
        out_ref[i, :XC] = (acc_x[0, i] + vy[i])[:, :N_VIR]
        v_x(i).wait_recv()
        out_ref[i, XC:] = (acc_y[0, i, :YC] + vx[i, :YC])[:, :N_VIR]
    for i in range(N_OCC):
        v_y(i).wait_send()
        v_x(i).wait_send()

    def sent(u, carry):
        for b in range(2):
            cross_x(u, b, b).wait_send()
            cross_y(u, b, b).wait_send()
        pair_x(u).wait_send()
        pair_y(u).wait_send()
        return carry

    lax.fori_loop(0, PAIRS, sent, 0)


def solution(mesh):
    def local_program(ints_blk, c_occ, c_vir):
        dma = pltpu.SemaphoreType.DMA
        xb, yb = (2, XC, 128), (2, YR, 128)
        out = pl.pallas_call(
            kernel,
            out_shape=jax.ShapeDtypeStruct((N_OCC, COLS, N_VIR), F32),
            in_specs=[pl.BlockSpec(memory_space=pl.ANY)] * 3,
            out_specs=pl.BlockSpec(memory_space=pltpu.VMEM),
            scratch_shapes=[
                pltpu.VMEM((N_OCC, N_R), BF16),
                pltpu.VMEM((N_VIR, N_R), BF16),
                pltpu.VMEM((SLOTS, N_Q, 120, N_R), BF16),
                pltpu.VMEM((8, 8 * N_OCC, 120), BF16),
                pltpu.VMEM((2, 2 * (XC + YR), 256), BF16),
                pltpu.VMEM((256, 256), BF16),
                pltpu.VMEM((N_OCC, 120, 128), F32),
                pltpu.VMEM((2, N_OCC, 128, 128), BF16),
                pltpu.VMEM((PAIRS, 2) + xb, BF16),
                pltpu.VMEM((PAIRS, 2) + yb, BF16),
                pltpu.VMEM((PAIRS, 2) + xb, BF16),
                pltpu.VMEM((PAIRS, 2) + yb, BF16),
                pltpu.VMEM((PAIRS,) + xb, BF16),
                pltpu.VMEM((PAIRS,) + yb, BF16),
                pltpu.VMEM((PAIRS, 2) + xb, BF16),
                pltpu.VMEM((PAIRS, 2) + yb, BF16),
                pltpu.VMEM((2, N_OCC, XC, 128), F32),
                pltpu.VMEM((2, N_OCC, YR, 128), F32),
                pltpu.VMEM((N_OCC, YR, 128), F32),
                pltpu.VMEM((N_OCC, XC, 128), F32),
                dma((SLOTS,)), dma((2,)), dma((PAIRS, 6)), dma((PAIRS, 6)),
                dma((2, N_OCC)), dma((2, N_OCC)),
            ],
            compiler_params=pltpu.CompilerParams(
                collective_id=0, has_side_effects=True,
                vmem_limit_bytes=36 * 1024 * 1024),
        )(ints_blk, pltpu.with_memory_space_constraint(c_occ.T, pltpu.HBM),
          pltpu.with_memory_space_constraint(c_vir.T, pltpu.HBM))
        return jnp.transpose(out, (0, 2, 1))

    return jax.shard_map(
        local_program,
        mesh=mesh,
        in_specs=(P(('frag', 'dev'), 'dev2', None, None), P('frag', None), P('frag', None)),
        out_specs=P(None, None, ('frag', 'dev2', 'dev')),
        check_vma=False,
    )
```

```python
import jax
import jax.numpy as jnp
from jax import lax
from jax.experimental import pallas as pl
from jax.experimental.pallas import tpu as pltpu
from jax.sharding import PartitionSpec as P

MESH = pl.DeviceIdType.MESH
F32 = jnp.float32
BF16 = jnp.bfloat16

N_P = 29
N_Q = 58
HALF = 29
N_R = 116
N_OCC = 6
N_VIR = 112
COLS = 84
XC = 42
YC = 42
XR = 48
YR = 48
SLOTS = 6
PAIRS = 15
LAG = 7


def kernel(a_ref, cot_ref, cvt_ref, out_ref, cot_v, cvt_v, abuf, lhs1, w2, cvb, cob, t1,
           lx, ly, xs, ys, px, py, xr, yr, acc_x, acc_y, vx, vy,
           a_sem, c_sem, send, recv, v_send, v_recv):
    frag = lax.axis_index("frag")
    y = lax.axis_index("dev2")
    dev = lax.axis_index("dev")
    x = dev // 2
    core = dev % 2
    partner = (frag, y, 2 * x + 1 - core)
    xnbr = [(frag, y, 2 * (1 - x) + b) for b in range(2)]
    ynbr = [(frag, 1 - y, 2 * x + b) for b in range(2)]

    small = [pltpu.make_async_copy(cot_ref, cot_v, c_sem.at[0]),
             pltpu.make_async_copy(cvt_ref, cvt_v, c_sem.at[1])]
    for copy in small:
        copy.start()

    def fetch(p, slot):
        return pltpu.make_async_copy(
            a_ref.at[p], abuf.at[slot, :, pl.ds(0, N_R)], a_sem.at[slot])

    for p in range(SLOTS):
        fetch(p, p).start()

    rest = jnp.zeros((PAIRS, 2, 2, YR - YC, 128), BF16)
    yr[:, :, :, YC:, :] = rest
    py[:, :, YC:, :] = rest[:, 0]
    rest = jnp.zeros((PAIRS, 2, 2, XR - XC, 128), BF16)
    xr[:, :, :, XC:, :] = rest
    px[:, :, XC:, :] = rest[:, 0]

    barrier = pltpu.get_barrier_semaphore()
    for peer in [partner] + xnbr + ynbr:
        pl.semaphore_signal(barrier, inc=1, device_id=peer, device_id_type=MESH)

    for s in range(SLOTS):
        abuf[s, :, N_R:, :] = jnp.zeros((N_Q, 4, N_R), BF16)
    acc_x[...] = jnp.zeros_like(acc_x)
    acc_y[...] = jnp.zeros_like(acc_y)
    lhs1[...] = jnp.zeros_like(lhs1)
    w2[...] = jnp.zeros_like(w2)
    cvb[...] = jnp.zeros_like(cvb)
    cob[...] = jnp.zeros_like(cob)
    for copy in small:
        copy.wait()

    cot = cot_v[...].astype(F32)
    rep = jnp.concatenate(
        [jnp.broadcast_to(cot[j:j + 1], (8, N_R)) for j in range(N_OCC)], axis=0)
    sub = lax.broadcasted_iota(jnp.int32, (8 * N_OCC, N_R), 0) % 8
    for m in range(8):
        lhs1[m, :, :N_R] = jnp.where(sub == m, rep, 0.0).astype(BF16)

    def first(slot, k):
        sums = []
        for g in range(4):
            total = None
            for m in range(min(8, HALF - 8 * g)):
                q = 8 * g + m
                left = jnp.pad(abuf[slot, q], ((0, 0), (0, 12)))
                right = jnp.pad(abuf[slot, HALF + q], ((0, 0), (0, 12)))
                term = jnp.dot(lhs1[m], jnp.concatenate([left, right], axis=1),
                               preferred_element_type=F32)
                total = term if total is None else total + term
            sums.append(total)
        for gp in range(2):
            for j in range(N_OCC):
                for h in range(2):
                    both = jnp.concatenate(
                        [sums[2 * gp + e][8 * j:8 * j + 8, 128 * h:128 * h + 128] for e in range(2)],
                        axis=0)
                    t1[j, k * 64 + h * 32 + gp * 16:k * 64 + h * 32 + gp * 16 + 16, :] = (
                        both.astype(BF16))

    def refill(p):
        @pl.when(p + SLOTS < N_P)
        def _():
            fetch(p + SLOTS, p % SLOTS).start()

    def stream(u):
        p = 2 * u
        fetch(p, p % SLOTS).wait()
        fetch(p + 1, (p + 1) % SLOTS).wait()

    def trip(u):
        p = 2 * u
        first(p % SLOTS, 0)
        first((p + 1) % SLOTS, 1)

    stream(0)
    trip(0)

    cvt = cvt_v[...].astype(F32)

    def put(xt, b, pieces):
        for kk in (0, 1):
            rows = jnp.concatenate(
                [cvt[lo:lo + n] if k == kk else jnp.zeros((n, N_R), F32) for n, lo, k in pieces]
                + [jnp.zeros((YR - YC, N_R), F32)], axis=0)
            head = jnp.concatenate([rows[:XC], jnp.zeros((XR - XC, N_R), F32)], axis=0)
            w2[xt, b * XR:(b + 1) * XR, kk * 128:kk * 128 + N_R] = head.astype(BF16)
            w2[xt, 2 * XR + b * YR:2 * XR + (b + 1) * YR, kk * 128:kk * 128 + N_R] = (
                rows[XC:].astype(BF16))

    put(0, 0, [(84, 0, 0)])
    put(0, 1, [(28, 84, 0), (56, 0, 1)])
    put(1, 0, [(56, 56, 0), (28, 0, 1)])
    put(1, 1, [(84, 28, 1)])

    cv = cvt.T
    for side in range(2):
        for h in range(2):
            lo = h * HALF
            low, high = cv[lo:lo + HALF], cv[N_Q + lo:N_Q + lo + HALF]
            part = jnp.where(y == side, low, high)
            part = jnp.concatenate([part, jnp.zeros((3, N_VIR), F32)], axis=0).astype(BF16)
            for k in range(2):
                cvb[pl.ds(side * 128 + k * 64 + h * 32, 32), k * 128:k * 128 + N_VIR] = part

    co = cot.T
    for i in range(N_OCC):
        cob[i, :N_R] = jnp.broadcast_to(co[:, i:i + 1], (N_R, 128))

    def second(u):
        for dx in range(2):
            xt = (x + dx) % 2
            rows = []
            for dy in range(2):
                j0 = 3 * ((y + dy) % 2) + xt
                rows.append(jnp.concatenate([t1[j0], t1[j0 + 1]], axis=1))
            half = lax.dot_general(w2[xt], jnp.concatenate(rows, axis=0), (((1,), (1,)), ((), ())),
                                   preferred_element_type=F32).astype(BF16)
            for b in range(2):
                for dy in range(2):
                    lane = slice(128 * dy, 128 * dy + 128)
                    (lx, xs)[dx][u, b, dy] = half[b * XR:(b + 1) * XR, lane]
                    (ly, ys)[dy][u, b, dx] = half[2 * XR + b * YR:2 * XR + (b + 1) * YR, lane]

    def remote(src, dst, s, r, peer):
        return pltpu.make_async_remote_copy(
            src_ref=src, dst_ref=dst, send_sem=s, recv_sem=r, device_id=peer, device_id_type=MESH)

    live_x, live = pl.ds(0, XC), pl.ds(0, YC)

    def cross_x(u, b, mark):
        return remote(xs.at[u, b, :, live_x], xr.at[u, core, :, live_x], send.at[u, b],
                      recv.at[u, mark], xnbr[b])

    def cross_y(u, b, mark):
        return remote(ys.at[u, b, :, live], yr.at[u, core, :, live], send.at[u, 2 + b],
                      recv.at[u, 2 + mark], ynbr[b])

    def pair_x(u):
        return remote(lx.at[u, 1 - core, :, live_x], px.at[u, :, live_x], send.at[u, 4],
                      recv.at[u, 4], partner)

    def pair_y(u):
        return remote(ly.at[u, 1 - core, :, live], py.at[u, :, live], send.at[u, 5],
                      recv.at[u, 5], partner)

    def send_pair(u):
        for b in range(2):
            cross_y(u, b, core).start()
            cross_x(u, b, core).start()
        pair_x(u).start()
        pair_y(u).start()

    def arrive(u):
        for b in range(2):
            cross_x(u, b, b).wait_recv()
            cross_y(u, b, b).wait_recv()
        pair_x(u).wait_recv()
        pair_y(u).wait_recv()

    def scales(u, source):
        p = source * N_P + 2 * u
        return [[jnp.broadcast_to(cob[i, pl.ds(p + e, 1), :], (8, 128)) for i in range(N_OCC)]
                for e in range(2)]

    def gather_x(acc, d, tiles, g, scale):
        for r in range(tiles):
            for i in range(N_OCC):
                v = acc[d, i, 8 * r:8 * r + 8]
                for rows, sc in zip(g, scale):
                    for e in range(2):
                        v = v + sc[e][i] * rows[8 * r:8 * r + 8, 128 * e:128 * e + 128]
                acc[d, i, 8 * r:8 * r + 8] = v

    def third(u, order=(0, 1)):
        flat = [lx[u, core], px[u], xr[u, 0], xr[u, 1]]
        from_x = [dev, 2 * x + 1 - core, 2 * (1 - x), 2 * (1 - x) + 1]
        ys_in = [jnp.concatenate([ly[u, core], yr[u, core]], axis=2),
                 jnp.concatenate([py[u], yr[u, 1 - core]], axis=2)]
        from_y = from_x[:2]
        gx = jnp.dot(jnp.concatenate([f[d] for d in order for f in flat], axis=0), cvb[:128],
                     preferred_element_type=F32)
        gy = jnp.dot(jnp.concatenate([f[d] for d in order for f in ys_in], axis=0), cvb[...],
                     preferred_element_type=F32)
        for n, d in enumerate(order):
            for s in range(0, 4, 2):
                at = (4 * n + s) * XR
                gather_x(acc_x, d, XR // 8, [gx[at:at + XR], gx[at + XR:at + 2 * XR]],
                         [scales(u, from_x[s]), scales(u, from_x[s + 1])])
            at = 2 * n * YR
            gather_x(acc_y, d, YR // 8, [gy[at:at + YR], gy[at + YR:at + 2 * YR]],
                     [scales(u, from_y[0]), scales(u, from_y[1])])

    def finish(u):
        second(u)
        send_pair(u)
        refill(2 * u)
        refill(2 * u + 1)

    pl.semaphore_wait(barrier, 5)
    finish(0)

    def early(u, carry):
        stream(u)
        trip(u)
        finish(u)
        return carry

    def late(u, carry):
        stream(u)
        arrive(u - LAG)
        third(u - LAG)
        trip(u)
        finish(u)
        return carry

    lax.fori_loop(1, LAG, early, 0)
    lax.fori_loop(LAG, PAIRS - 1, late, 0)

    last = PAIRS - 1
    t1[:, 64:, :] = jnp.zeros((N_OCC, 64, 128), BF16)
    fetch(N_P - 1, (N_P - 1) % SLOTS).wait()
    first((N_P - 1) % SLOTS, 0)
    second(last)
    send_pair(last)

    def drain(u, carry):
        arrive(u)
        third(u)
        return carry

    lax.fori_loop(last - LAG, last, drain, 0)
    arrive(last)
    third(last, (1, 0))

    def v_y(i):
        return remote(acc_x.at[1, i, live_x], vy.at[i, live_x], v_send.at[0, i], v_recv.at[0, i],
                      (frag, 1 - y, dev))

    def v_x(i):
        return remote(acc_y.at[1, i, live], vx.at[i, live], v_send.at[1, i], v_recv.at[1, i],
                      (frag, y, 2 * (1 - x) + core))

    for i in range(N_OCC):
        v_y(i).start()
        v_x(i).start()
    for i in range(N_OCC):
        v_y(i).wait_recv()
        out_ref[i, :XC] = (acc_x[0, i, :XC] + vy[i, :XC])[:, :N_VIR]
        v_x(i).wait_recv()
        out_ref[i, XC:] = (acc_y[0, i, :YC] + vx[i, :YC])[:, :N_VIR]
    for i in range(N_OCC):
        v_y(i).wait_send()
        v_x(i).wait_send()

    def sent(u, carry):
        for b in range(2):
            cross_x(u, b, b).wait_send()
            cross_y(u, b, b).wait_send()
        pair_x(u).wait_send()
        pair_y(u).wait_send()
        return carry

    lax.fori_loop(0, PAIRS, sent, 0)


def solution(mesh):
    def local_program(ints_blk, c_occ, c_vir):
        dma = pltpu.SemaphoreType.DMA
        xb, yb = (2, XR, 128), (2, YR, 128)
        out = pl.pallas_call(
            kernel,
            out_shape=jax.ShapeDtypeStruct((N_OCC, COLS, N_VIR), F32),
            in_specs=[pl.BlockSpec(memory_space=pl.ANY)] * 3,
            out_specs=pl.BlockSpec(memory_space=pltpu.VMEM),
            scratch_shapes=[
                pltpu.VMEM((N_OCC, N_R), BF16),
                pltpu.VMEM((N_VIR, N_R), BF16),
                pltpu.VMEM((SLOTS, N_Q, 120, N_R), BF16),
                pltpu.VMEM((8, 8 * N_OCC, 120), BF16),
                pltpu.VMEM((2, 2 * (XR + YR), 256), BF16),
                pltpu.VMEM((256, 256), BF16),
                pltpu.VMEM((N_OCC, 120, 128), F32),
                pltpu.VMEM((N_OCC, 128, 128), BF16),
                pltpu.VMEM((PAIRS, 2) + xb, BF16),
                pltpu.VMEM((PAIRS, 2) + yb, BF16),
                pltpu.VMEM((PAIRS, 2) + xb, BF16),
                pltpu.VMEM((PAIRS, 2) + yb, BF16),
                pltpu.VMEM((PAIRS,) + xb, BF16),
                pltpu.VMEM((PAIRS,) + yb, BF16),
                pltpu.VMEM((PAIRS, 2) + xb, BF16),
                pltpu.VMEM((PAIRS, 2) + yb, BF16),
                pltpu.VMEM((2, N_OCC, XR, 128), F32),
                pltpu.VMEM((2, N_OCC, YR, 128), F32),
                pltpu.VMEM((N_OCC, YR, 128), F32),
                pltpu.VMEM((N_OCC, XR, 128), F32),
                dma((SLOTS,)), dma((2,)), dma((PAIRS, 6)), dma((PAIRS, 6)),
                dma((2, N_OCC)), dma((2, N_OCC)),
            ],
            compiler_params=pltpu.CompilerParams(
                collective_id=0, has_side_effects=True,
                vmem_limit_bytes=36 * 1024 * 1024),
        )(ints_blk, pltpu.with_memory_space_constraint(c_occ.T, pltpu.HBM),
          pltpu.with_memory_space_constraint(c_vir.T, pltpu.HBM))
        return jnp.transpose(out, (0, 2, 1))

    return jax.shard_map(
        local_program,
        mesh=mesh,
        in_specs=(P(('frag', 'dev'), 'dev2', None, None), P('frag', None), P('frag', None)),
        out_specs=P(None, None, ('frag', 'dev2', 'dev')),
        check_vma=False,
    )
```

```python
import jax
import jax.numpy as jnp
from jax import lax
from jax.experimental import pallas as pl
from jax.experimental.pallas import tpu as pltpu
from jax.sharding import PartitionSpec as P

MESH = pl.DeviceIdType.MESH
F32 = jnp.float32
BF16 = jnp.bfloat16

N_P = 29
N_Q = 58
HALF = 29
N_R = 116
N_OCC = 6
N_VIR = 112
COLS = 84
XC = 42
YC = 42
XR = 48
YR = 48
SLOTS = 6
PAIRS = 15
LAG = 10


def kernel(a_ref, cot_ref, cvt_ref, out_ref, cot_v, cvt_v, abuf, lhs1, w2, cvb, cob, t1,
           lx, ly, xs, ys, px, py, xr, yr, acc_x, acc_y, vx, vy,
           a_sem, c_sem, send, recv, v_send, v_recv):
    frag = lax.axis_index("frag")
    y = lax.axis_index("dev2")
    dev = lax.axis_index("dev")
    x = dev // 2
    core = dev % 2
    partner = (frag, y, 2 * x + 1 - core)
    xnbr = [(frag, y, 2 * (1 - x) + b) for b in range(2)]
    ynbr = [(frag, 1 - y, 2 * x + b) for b in range(2)]

    small = [pltpu.make_async_copy(cot_ref, cot_v, c_sem.at[0]),
             pltpu.make_async_copy(cvt_ref, cvt_v, c_sem.at[1])]
    for copy in small:
        copy.start()

    def fetch(p, slot):
        return pltpu.make_async_copy(
            a_ref.at[p], abuf.at[slot, :, pl.ds(0, N_R)], a_sem.at[slot])

    for p in range(SLOTS):
        fetch(p, p).start()

    rest = jnp.zeros((PAIRS, 2, 2, YR - YC, 128), BF16)
    yr[:, :, :, YC:, :] = rest
    py[:, :, YC:, :] = rest[:, 0]
    rest = jnp.zeros((PAIRS, 2, 2, XR - XC, 128), BF16)
    xr[:, :, :, XC:, :] = rest
    px[:, :, XC:, :] = rest[:, 0]

    barrier = pltpu.get_barrier_semaphore()
    for peer in [partner] + xnbr + ynbr:
        pl.semaphore_signal(barrier, inc=1, device_id=peer, device_id_type=MESH)

    for s in range(SLOTS):
        abuf[s, :, N_R:, :] = jnp.zeros((N_Q, 4, N_R), BF16)
    acc_x[...] = jnp.zeros_like(acc_x)
    acc_y[...] = jnp.zeros_like(acc_y)
    lhs1[...] = jnp.zeros_like(lhs1)
    w2[...] = jnp.zeros_like(w2)
    cvb[...] = jnp.zeros_like(cvb)
    cob[...] = jnp.zeros_like(cob)
    for copy in small:
        copy.wait()

    cot = cot_v[...].astype(F32)
    rep = jnp.concatenate(
        [jnp.broadcast_to(cot[j:j + 1], (8, N_R)) for j in range(N_OCC)], axis=0)
    sub = lax.broadcasted_iota(jnp.int32, (8 * N_OCC, N_R), 0) % 8
    for m in range(8):
        lhs1[m, :, :N_R] = jnp.where(sub == m, rep, 0.0).astype(BF16)

    def first(slot, k):
        sums = []
        for g in range(4):
            total = None
            for m in range(min(8, HALF - 8 * g)):
                q = 8 * g + m
                left = jnp.pad(abuf[slot, q], ((0, 0), (0, 12)))
                right = jnp.pad(abuf[slot, HALF + q], ((0, 0), (0, 12)))
                term = jnp.dot(lhs1[m], jnp.concatenate([left, right], axis=1),
                               preferred_element_type=F32)
                total = term if total is None else total + term
            sums.append(total)
        for gp in range(2):
            for j in range(N_OCC):
                for h in range(2):
                    both = jnp.concatenate(
                        [sums[2 * gp + e][8 * j:8 * j + 8, 128 * h:128 * h + 128] for e in range(2)],
                        axis=0)
                    t1[j, k * 64 + h * 32 + gp * 16:k * 64 + h * 32 + gp * 16 + 16, :] = (
                        both.astype(BF16))

    def refill(p):
        @pl.when(p + SLOTS < N_P)
        def _():
            fetch(p + SLOTS, p % SLOTS).start()

    def stream(u):
        p = 2 * u
        fetch(p, p % SLOTS).wait()
        fetch(p + 1, (p + 1) % SLOTS).wait()

    def trip(u):
        p = 2 * u
        first(p % SLOTS, 0)
        first((p + 1) % SLOTS, 1)

    stream(0)
    trip(0)

    cvt = cvt_v[...].astype(F32)

    def put(xt, b, pieces):
        for kk in (0, 1):
            rows = jnp.concatenate(
                [cvt[lo:lo + n] if k == kk else jnp.zeros((n, N_R), F32) for n, lo, k in pieces]
                + [jnp.zeros((YR - YC, N_R), F32)], axis=0)
            head = jnp.concatenate([rows[:XC], jnp.zeros((XR - XC, N_R), F32)], axis=0)
            w2[xt, b * XR:(b + 1) * XR, kk * 128:kk * 128 + N_R] = head.astype(BF16)
            w2[xt, 2 * XR + b * YR:2 * XR + (b + 1) * YR, kk * 128:kk * 128 + N_R] = (
                rows[XC:].astype(BF16))

    put(0, 0, [(84, 0, 0)])
    put(0, 1, [(28, 84, 0), (56, 0, 1)])
    put(1, 0, [(56, 56, 0), (28, 0, 1)])
    put(1, 1, [(84, 28, 1)])

    cv = cvt.T
    for side in range(2):
        for h in range(2):
            lo = h * HALF
            low, high = cv[lo:lo + HALF], cv[N_Q + lo:N_Q + lo + HALF]
            part = jnp.where(y == side, low, high)
            part = jnp.concatenate([part, jnp.zeros((3, N_VIR), F32)], axis=0).astype(BF16)
            for k in range(2):
                cvb[pl.ds(side * 128 + k * 64 + h * 32, 32), k * 128:k * 128 + N_VIR] = part

    co = cot.T
    for i in range(N_OCC):
        cob[i, :N_R] = jnp.broadcast_to(co[:, i:i + 1], (N_R, 128))

    def second(u):
        for dx in range(2):
            xt = (x + dx) % 2
            rows = []
            for dy in range(2):
                j0 = 3 * ((y + dy) % 2) + xt
                rows.append(jnp.concatenate([t1[j0], t1[j0 + 1]], axis=1))
            half = lax.dot_general(w2[xt], jnp.concatenate(rows, axis=0), (((1,), (1,)), ((), ())),
                                   preferred_element_type=F32).astype(BF16)
            for b in range(2):
                for dy in range(2):
                    lane = slice(128 * dy, 128 * dy + 128)
                    (lx, xs)[dx][u, b, dy] = half[b * XR:(b + 1) * XR, lane]
                    (ly, ys)[dy][u, b, dx] = half[2 * XR + b * YR:2 * XR + (b + 1) * YR, lane]

    def remote(src, dst, s, r, peer):
        return pltpu.make_async_remote_copy(
            src_ref=src, dst_ref=dst, send_sem=s, recv_sem=r, device_id=peer, device_id_type=MESH)

    live_x, live = pl.ds(0, XC), pl.ds(0, YC)

    def cross_x(u, b, mark):
        return remote(xs.at[u, b, :, live_x], xr.at[u, core, :, live_x], send.at[u, b],
                      recv.at[u, mark], xnbr[b])

    def cross_y(u, b, mark):
        return remote(ys.at[u, b, :, live], yr.at[u, core, :, live], send.at[u, 2 + b],
                      recv.at[u, 2 + mark], ynbr[b])

    def pair_x(u):
        return remote(lx.at[u, 1 - core, :, live_x], px.at[u, :, live_x], send.at[u, 4],
                      recv.at[u, 4], partner)

    def pair_y(u):
        return remote(ly.at[u, 1 - core, :, live], py.at[u, :, live], send.at[u, 5],
                      recv.at[u, 5], partner)

    def send_pair(u):
        for b in range(2):
            cross_y(u, b, core).start()
            cross_x(u, b, core).start()
        pair_x(u).start()
        pair_y(u).start()

    def arrive(u):
        for b in range(2):
            cross_x(u, b, b).wait_recv()
            cross_y(u, b, b).wait_recv()
        pair_x(u).wait_recv()
        pair_y(u).wait_recv()

    def scales(u, source):
        p = source * N_P + 2 * u
        return [[jnp.broadcast_to(cob[i, pl.ds(p + e, 1), :], (8, 128)) for i in range(N_OCC)]
                for e in range(2)]

    def gather_x(acc, d, tiles, g, scale):
        for r in range(tiles):
            for i in range(N_OCC):
                v = acc[d, i, 8 * r:8 * r + 8]
                for rows, sc in zip(g, scale):
                    for e in range(2):
                        v = v + sc[e][i] * rows[8 * r:8 * r + 8, 128 * e:128 * e + 128]
                acc[d, i, 8 * r:8 * r + 8] = v

    def third(u, order=(0, 1)):
        flat = [lx[u, core], px[u], xr[u, 0], xr[u, 1]]
        from_x = [dev, 2 * x + 1 - core, 2 * (1 - x), 2 * (1 - x) + 1]
        ys_in = [jnp.concatenate([ly[u, core], yr[u, core]], axis=2),
                 jnp.concatenate([py[u], yr[u, 1 - core]], axis=2)]
        from_y = from_x[:2]
        gx = jnp.dot(jnp.concatenate([f[d] for d in order for f in flat], axis=0), cvb[:128],
                     preferred_element_type=F32)
        gy = jnp.dot(jnp.concatenate([f[d] for d in order for f in ys_in], axis=0), cvb[...],
                     preferred_element_type=F32)
        for n, d in enumerate(order):
            for s in range(0, 4, 2):
                at = (4 * n + s) * XR
                gather_x(acc_x, d, XR // 8, [gx[at:at + XR], gx[at + XR:at + 2 * XR]],
                         [scales(u, from_x[s]), scales(u, from_x[s + 1])])
            at = 2 * n * YR
            gather_x(acc_y, d, YR // 8, [gy[at:at + YR], gy[at + YR:at + 2 * YR]],
                     [scales(u, from_y[0]), scales(u, from_y[1])])

    def finish(u):
        second(u)
        send_pair(u)
        refill(2 * u)
        refill(2 * u + 1)

    pl.semaphore_wait(barrier, 5)
    finish(0)

    def early(u, carry):
        stream(u)
        trip(u)
        finish(u)
        return carry

    def late(u, carry):
        stream(u)
        arrive(u - LAG)
        third(u - LAG)
        trip(u)
        finish(u)
        return carry

    lax.fori_loop(1, LAG, early, 0)
    lax.fori_loop(LAG, PAIRS - 1, late, 0)

    last = PAIRS - 1
    t1[:, 64:, :] = jnp.zeros((N_OCC, 64, 128), BF16)
    fetch(N_P - 1, (N_P - 1) % SLOTS).wait()
    first((N_P - 1) % SLOTS, 0)
    second(last)
    send_pair(last)

    def drain(u, carry):
        arrive(u)
        third(u)
        return carry

    lax.fori_loop(last - LAG, last, drain, 0)
    arrive(last)
    third(last, (1, 0))

    def v_y(i):
        return remote(acc_x.at[1, i, live_x], vy.at[i, live_x], v_send.at[0, i], v_recv.at[0, i],
                      (frag, 1 - y, dev))

    def v_x(i):
        return remote(acc_y.at[1, i, live], vx.at[i, live], v_send.at[1, i], v_recv.at[1, i],
                      (frag, y, 2 * (1 - x) + core))

    for i in range(N_OCC):
        v_y(i).start()
        v_x(i).start()
    for i in range(N_OCC):
        v_y(i).wait_recv()
        out_ref[i, :XC] = (acc_x[0, i, :XC] + vy[i, :XC])[:, :N_VIR]
        v_x(i).wait_recv()
        out_ref[i, XC:] = (acc_y[0, i, :YC] + vx[i, :YC])[:, :N_VIR]
    for i in range(N_OCC):
        v_y(i).wait_send()
        v_x(i).wait_send()

    def sent(u, carry):
        for b in range(2):
            cross_x(u, b, b).wait_send()
            cross_y(u, b, b).wait_send()
        pair_x(u).wait_send()
        pair_y(u).wait_send()
        return carry

    lax.fori_loop(0, PAIRS, sent, 0)


def solution(mesh):
    def local_program(ints_blk, c_occ, c_vir):
        dma = pltpu.SemaphoreType.DMA
        xb, yb = (2, XR, 128), (2, YR, 128)
        out = pl.pallas_call(
            kernel,
            out_shape=jax.ShapeDtypeStruct((N_OCC, COLS, N_VIR), F32),
            in_specs=[pl.BlockSpec(memory_space=pl.ANY)] * 3,
            out_specs=pl.BlockSpec(memory_space=pltpu.VMEM),
            scratch_shapes=[
                pltpu.VMEM((N_OCC, N_R), BF16),
                pltpu.VMEM((N_VIR, N_R), BF16),
                pltpu.VMEM((SLOTS, N_Q, 120, N_R), BF16),
                pltpu.VMEM((8, 8 * N_OCC, 120), BF16),
                pltpu.VMEM((2, 2 * (XR + YR), 256), BF16),
                pltpu.VMEM((256, 256), BF16),
                pltpu.VMEM((N_OCC, 120, 128), F32),
                pltpu.VMEM((N_OCC, 128, 128), BF16),
                pltpu.VMEM((PAIRS, 2) + xb, BF16),
                pltpu.VMEM((PAIRS, 2) + yb, BF16),
                pltpu.VMEM((PAIRS, 2) + xb, BF16),
                pltpu.VMEM((PAIRS, 2) + yb, BF16),
                pltpu.VMEM((PAIRS,) + xb, BF16),
                pltpu.VMEM((PAIRS,) + yb, BF16),
                pltpu.VMEM((PAIRS, 2) + xb, BF16),
                pltpu.VMEM((PAIRS, 2) + yb, BF16),
                pltpu.VMEM((2, N_OCC, XR, 128), F32),
                pltpu.VMEM((2, N_OCC, YR, 128), F32),
                pltpu.VMEM((N_OCC, YR, 128), F32),
                pltpu.VMEM((N_OCC, XR, 128), F32),
                dma((SLOTS,)), dma((2,)), dma((PAIRS, 6)), dma((PAIRS, 6)),
                dma((2, N_OCC)), dma((2, N_OCC)),
            ],
            compiler_params=pltpu.CompilerParams(
                collective_id=0, has_side_effects=True,
                vmem_limit_bytes=36 * 1024 * 1024),
        )(ints_blk, pltpu.with_memory_space_constraint(c_occ.T, pltpu.HBM),
          pltpu.with_memory_space_constraint(c_vir.T, pltpu.HBM))
        return jnp.transpose(out, (0, 2, 1))

    return jax.shard_map(
        local_program,
        mesh=mesh,
        in_specs=(P(('frag', 'dev'), 'dev2', None, None), P('frag', None), P('frag', None)),
        out_specs=P(None, None, ('frag', 'dev2', 'dev')),
        check_vma=False,
    )
```

```python
import jax
import jax.numpy as jnp
from jax import lax
from jax.experimental import pallas as pl
from jax.experimental.pallas import tpu as pltpu
from jax.sharding import PartitionSpec as P

MESH = pl.DeviceIdType.MESH
F32 = jnp.float32
BF16 = jnp.bfloat16

N_P = 29
N_Q = 58
HALF = 29
N_R = 116
N_OCC = 6
N_VIR = 112
COLS = 84
XC = 40
YC = 44
YR = 48
SLOTS = 6
PAIRS = 15
ACC_X = 0
ACC_Y = ACC_X + 2 * N_OCC * XC
COEF = ACC_Y + 2 * N_OCC * YR
LAG = 6


def kernel(a_ref, cot_ref, cvt_ref, out_ref, cot_v, cvt_v, abuf, lhs1, w2, cvb, cob, t1,
           lx, ly, xs, ys, px, py, xr, yr, pool, vx, vy,
           a_sem, c_sem, send, recv, v_send, v_recv):
    frag = lax.axis_index("frag")
    y = lax.axis_index("dev2")
    dev = lax.axis_index("dev")
    x = dev // 2
    core = dev % 2
    partner = (frag, y, 2 * x + 1 - core)
    xnbr = [(frag, y, 2 * (1 - x) + b) for b in range(2)]
    ynbr = [(frag, 1 - y, 2 * x + b) for b in range(2)]

    small = [pltpu.make_async_copy(cot_ref, cot_v, c_sem.at[0]),
             pltpu.make_async_copy(cvt_ref, cvt_v, c_sem.at[1])]
    for copy in small:
        copy.start()

    def fetch(p, slot):
        return pltpu.make_async_copy(
            a_ref.at[p], abuf.at[slot, :, pl.ds(0, N_R)], a_sem.at[slot])

    for p in range(SLOTS):
        fetch(p, p).start()

    rest = jnp.zeros((PAIRS, 2, 2, YR - YC, 128), BF16)
    yr[:, :, :, YC:, :] = rest
    py[:, :, YC:, :] = rest[:, 0]

    barrier = pltpu.get_barrier_semaphore()
    for peer in [partner] + xnbr + ynbr:
        pl.semaphore_signal(barrier, inc=1, device_id=peer, device_id_type=MESH)

    for s in range(SLOTS):
        abuf[s, :, N_R:, :] = jnp.zeros((N_Q, 4, N_R), BF16)
    pool[...] = jnp.zeros_like(pool)
    lhs1[...] = jnp.zeros_like(lhs1)
    w2[...] = jnp.zeros_like(w2)
    cvb[...] = jnp.zeros_like(cvb)
    cob[...] = jnp.zeros_like(cob)
    for copy in small:
        copy.wait()

    cot = cot_v[...].astype(F32)
    rep = jnp.concatenate(
        [jnp.broadcast_to(cot[j:j + 1], (8, N_R)) for j in range(N_OCC)], axis=0)
    sub = lax.broadcasted_iota(jnp.int32, (8 * N_OCC, N_R), 0) % 8
    for m in range(8):
        lhs1[m, :, :N_R] = jnp.where(sub == m, rep, 0.0).astype(BF16)

    cvt = cvt_v[...].astype(F32)

    def put(xt, b, pieces):
        for kk in (0, 1):
            rows = jnp.concatenate(
                [cvt[lo:lo + n] if k == kk else jnp.zeros((n, N_R), F32) for n, lo, k in pieces]
                + [jnp.zeros((YR - YC, N_R), F32)], axis=0).astype(BF16)
            w2[xt, pl.ds(b * XC, XC), kk * 128:kk * 128 + N_R] = rows[:XC]
            w2[xt, pl.ds(2 * XC + b * YR, YR), kk * 128:kk * 128 + N_R] = rows[XC:]

    put(0, 0, [(84, 0, 0)])
    put(0, 1, [(28, 84, 0), (56, 0, 1)])
    put(1, 0, [(56, 56, 0), (28, 0, 1)])
    put(1, 1, [(84, 28, 1)])

    cv = cvt.T
    for side in range(2):
        for h in range(2):
            lo = h * HALF
            low, high = cv[lo:lo + HALF], cv[N_Q + lo:N_Q + lo + HALF]
            part = jnp.where(y == side, low, high)
            part = jnp.concatenate([part, jnp.zeros((3, N_VIR), F32)], axis=0).astype(BF16)
            for k in range(2):
                cvb[pl.ds(side * 128 + k * 64 + h * 32, 32), k * 128:k * 128 + N_VIR] = part

    co = cot.T
    for i in range(N_OCC):
        rows = jnp.broadcast_to(co[:, i:i + 1], (N_R, 128))
        cob[i * 120:i * 120 + N_R, :] = rows
        pool[COEF + i * 120:COEF + i * 120 + N_R, :] = rows

    def first(slot, par, k):
        sums = []
        for g in range(4):
            total = None
            for m in range(min(8, HALF - 8 * g)):
                q = 8 * g + m
                left = jnp.pad(abuf[slot, q], ((0, 0), (0, 12)))
                right = jnp.pad(abuf[slot, HALF + q], ((0, 0), (0, 12)))
                term = jnp.dot(lhs1[m], jnp.concatenate([left, right], axis=1),
                               preferred_element_type=F32)
                total = term if total is None else total + term
            sums.append(total)
        for gp in range(2):
            for j in range(N_OCC):
                for h in range(2):
                    both = jnp.concatenate(
                        [sums[2 * gp + e][8 * j:8 * j + 8, 128 * h:128 * h + 128] for e in range(2)],
                        axis=0)
                    t1[par, j, k * 64 + h * 32 + gp * 16:k * 64 + h * 32 + gp * 16 + 16, :] = (
                        both.astype(BF16))

    def second(par, u):
        for dx in range(2):
            xt = (x + dx) % 2
            rows = []
            for dy in range(2):
                j0 = 3 * ((y + dy) % 2) + xt
                rows.append(jnp.concatenate([t1[par, j0], t1[par, j0 + 1]], axis=1))
            half = lax.dot_general(w2[xt], jnp.concatenate(rows, axis=0), (((1,), (1,)), ((), ())),
                                   preferred_element_type=F32).astype(BF16)
            for b in range(2):
                for dy in range(2):
                    lane = slice(128 * dy, 128 * dy + 128)
                    (lx, xs)[dx][u, b, dy] = half[b * XC:(b + 1) * XC, lane]
                    (ly, ys)[dy][u, b, dx] = half[2 * XC + b * YR:2 * XC + (b + 1) * YR, lane]

    def remote(src, dst, s, r, peer):
        return pltpu.make_async_remote_copy(
            src_ref=src, dst_ref=dst, send_sem=s, recv_sem=r, device_id=peer, device_id_type=MESH)

    live = pl.ds(0, YC)

    def cross_x(u, b, mark):
        return remote(xs.at[u, b], xr.at[u, core], send.at[u, b], recv.at[u, mark], xnbr[b])

    def cross_y(u, b, mark):
        return remote(ys.at[u, b, :, live], yr.at[u, core, :, live], send.at[u, 2 + b],
                      recv.at[u, 2 + mark], ynbr[b])

    def pair_x(u):
        return remote(lx.at[u, 1 - core], px.at[u], send.at[u, 4], recv.at[u, 4], partner)

    def pair_y(u):
        return remote(ly.at[u, 1 - core, :, live], py.at[u, :, live], send.at[u, 5],
                      recv.at[u, 5], partner)

    def send_pair(u):
        for b in range(2):
            cross_y(u, b, core).start()
            cross_x(u, b, core).start()
        pair_x(u).start()
        pair_y(u).start()

    def arrive(u):
        for b in range(2):
            cross_x(u, b, b).wait_recv()
            cross_y(u, b, b).wait_recv()
        pair_x(u).wait_recv()
        pair_y(u).wait_recv()

    def scales(u, source, table, base):
        p = source * N_P + 2 * u
        return [[jnp.broadcast_to(table[pl.ds(base + i * 120 + p + e, 1), :], (8, 128))
                 for i in range(N_OCC)] for e in range(2)]

    def gather(base, tiles, g, source, u, paced):
        for half in (0, 3):
            for lo, hi in ((0, tiles // 2), (tiles // 2, tiles)) if paced else ((0, tiles),):
                table, at = (pool, COEF) if paced else (cob, 0)
                scale = [scales(u, s, table, at) for s in source]
                for r in range(lo, hi):
                    for i in range(half, half + 3):
                        row = base + i * tiles * 8 + 8 * r
                        v = pool[row:row + 8, :]
                        for rows, sc in zip(g, scale):
                            for e in range(2):
                                v = v + sc[e][i] * rows[8 * r:8 * r + 8, 128 * e:128 * e + 128]
                        pool[row:row + 8, :] = v

    from_x = [dev, 2 * x + 1 - core, 2 * (1 - x), 2 * (1 - x) + 1]

    def third(u, paced, order=(0, 1)):
        flat = [lx[u, core], px[u], xr[u, 0], xr[u, 1]]
        ys_in = [jnp.concatenate([ly[u, core], yr[u, core]], axis=2),
                 jnp.concatenate([py[u], yr[u, 1 - core]], axis=2)]
        gx = jnp.dot(jnp.concatenate([f[d] for d in order for f in flat], axis=0), cvb[:128],
                     preferred_element_type=F32)
        gy = jnp.dot(jnp.concatenate([f[d] for d in order for f in ys_in], axis=0), cvb[...],
                     preferred_element_type=F32)
        for n, d in enumerate(order):
            for s in range(0, 4, 2):
                at = (4 * n + s) * XC
                gather(ACC_X + d * N_OCC * XC, XC // 8, [gx[at:at + XC], gx[at + XC:at + 2 * XC]],
                       from_x[s:s + 2], u, paced)
            at = 2 * n * YR
            gather(ACC_Y + d * N_OCC * YR, YR // 8, [gy[at:at + YR], gy[at + YR:at + 2 * YR]],
                   from_x[:2], u, paced)

    def refill(p):
        @pl.when(p + SLOTS < N_P)
        def _():
            fetch(p + SLOTS, p % SLOTS).start()

    def stream(u):
        p = 2 * u
        fetch(p, p % SLOTS).wait()
        fetch(p + 1, (p + 1) % SLOTS).wait()

    def trip(u):
        p = 2 * u
        first(p % SLOTS, u % 2, 0)
        first((p + 1) % SLOTS, u % 2, 1)

    def after(u):
        refill(2 * u)
        refill(2 * u + 1)

    stream(0)
    trip(0)
    after(0)
    pl.semaphore_wait(barrier, 5)

    def early(u, carry):
        stream(u)
        second((u + 1) % 2, u - 1)
        trip(u)
        send_pair(u - 1)
        after(u)
        return carry

    def late(u, carry):
        stream(u)
        arrive(u - LAG)
        third(u - LAG, True)
        second((u + 1) % 2, u - 1)
        trip(u)
        send_pair(u - 1)
        after(u)
        return carry

    lax.fori_loop(1, LAG, early, 0)
    lax.fori_loop(LAG, PAIRS - 1, late, 0)

    last = PAIRS - 1
    second(1, last - 1)
    send_pair(last - 1)
    t1[0, :, 64:, :] = jnp.zeros((N_OCC, 64, 128), BF16)
    fetch(N_P - 1, (N_P - 1) % SLOTS).wait()
    first((N_P - 1) % SLOTS, 0, 0)
    second(0, last)
    send_pair(last)

    def drain(n, carry):
        u = last - LAG + 2 * n
        arrive(u)
        arrive(u + 1)
        third(u, False)
        third(u + 1, False)
        return carry

    lax.fori_loop(0, LAG // 2, drain, 0)
    arrive(last)
    third(last, False, (1, 0))

    def acc_x(d, i):
        return pl.ds(ACC_X + (d * N_OCC + i) * XC, XC)

    def acc_y(d, i):
        return pl.ds(ACC_Y + (d * N_OCC + i) * YR, YC)

    def v_y(i):
        return remote(pool.at[acc_x(1, i)], vy.at[i], v_send.at[0, i], v_recv.at[0, i], (frag, 1 - y, dev))

    def v_x(i):
        return remote(pool.at[acc_y(1, i)], vx.at[i, live], v_send.at[1, i], v_recv.at[1, i],
                      (frag, y, 2 * (1 - x) + core))

    for i in range(N_OCC):
        v_y(i).start()
        v_x(i).start()
    for i in range(N_OCC):
        v_y(i).wait_recv()
        out_ref[i, :XC] = (pool[acc_x(0, i), :] + vy[i])[:, :N_VIR]
        v_x(i).wait_recv()
        out_ref[i, XC:] = (pool[acc_y(0, i), :] + vx[i, :YC])[:, :N_VIR]
    for i in range(N_OCC):
        v_y(i).wait_send()
        v_x(i).wait_send()

    def sent(u, carry):
        for b in range(2):
            cross_x(u, b, b).wait_send()
            cross_y(u, b, b).wait_send()
        pair_x(u).wait_send()
        pair_y(u).wait_send()
        return carry

    lax.fori_loop(0, PAIRS, sent, 0)


def solution(mesh):
    def local_program(ints_blk, c_occ, c_vir):
        dma = pltpu.SemaphoreType.DMA
        xb, yb = (2, XC, 128), (2, YR, 128)
        out = pl.pallas_call(
            kernel,
            out_shape=jax.ShapeDtypeStruct((N_OCC, COLS, N_VIR), F32),
            in_specs=[pl.BlockSpec(memory_space=pl.ANY)] * 3,
            out_specs=pl.BlockSpec(memory_space=pltpu.VMEM),
            scratch_shapes=[
                pltpu.VMEM((N_OCC, N_R), BF16),
                pltpu.VMEM((N_VIR, N_R), BF16),
                pltpu.VMEM((SLOTS, N_Q, 120, N_R), BF16),
                pltpu.VMEM((8, 8 * N_OCC, 120), BF16),
                pltpu.VMEM((2, 2 * (XC + YR), 256), BF16),
                pltpu.VMEM((256, 256), BF16),
                pltpu.VMEM((N_OCC * 120, 128), F32),
                pltpu.VMEM((2, N_OCC, 128, 128), BF16),
                pltpu.VMEM((PAIRS, 2) + xb, BF16),
                pltpu.VMEM((PAIRS, 2) + yb, BF16),
                pltpu.VMEM((PAIRS, 2) + xb, BF16),
                pltpu.VMEM((PAIRS, 2) + yb, BF16),
                pltpu.VMEM((PAIRS,) + xb, BF16),
                pltpu.VMEM((PAIRS,) + yb, BF16),
                pltpu.VMEM((PAIRS, 2) + xb, BF16),
                pltpu.VMEM((PAIRS, 2) + yb, BF16),
                pltpu.VMEM((COEF + N_OCC * 120, 128), F32),
                pltpu.VMEM((N_OCC, YR, 128), F32),
                pltpu.VMEM((N_OCC, XC, 128), F32),
                dma((SLOTS,)), dma((2,)), dma((PAIRS, 6)), dma((PAIRS, 6)),
                dma((2, N_OCC)), dma((2, N_OCC)),
            ],
            compiler_params=pltpu.CompilerParams(
                collective_id=0, has_side_effects=True,
                vmem_limit_bytes=36 * 1024 * 1024),
        )(ints_blk, pltpu.with_memory_space_constraint(c_occ.T, pltpu.HBM),
          pltpu.with_memory_space_constraint(c_vir.T, pltpu.HBM))
        return jnp.transpose(out, (0, 2, 1))

    return jax.shard_map(
        local_program,
        mesh=mesh,
        in_specs=(P(('frag', 'dev'), 'dev2', None, None), P('frag', None), P('frag', None)),
        out_specs=P(None, None, ('frag', 'dev2', 'dev')),
        check_vma=False,
    )
```

```python
import jax
import jax.numpy as jnp
from jax import lax
from jax.experimental import pallas as pl
from jax.experimental.pallas import tpu as pltpu
from jax.sharding import PartitionSpec as P

MESH = pl.DeviceIdType.MESH
F32 = jnp.float32
BF16 = jnp.bfloat16

N_P = 29
N_Q = 58
HALF = 29
N_R = 116
N_OCC = 6
N_VIR = 112
COLS = 84
XC = 42
YC = 42
XR = 48
YR = 48
SLOTS = 6
PAIRS = 15
ACC_X = 0
ACC_Y = ACC_X + 2 * N_OCC * XR
COEF = ACC_Y + 2 * N_OCC * YR
LAG = 10


def kernel(a_ref, cot_ref, cvt_ref, out_ref, cot_v, cvt_v, abuf, lhs1, w2, cvb, cob, t1,
           lx, ly, xs, ys, px, py, xr, yr, pool, vx, vy,
           a_sem, c_sem, send, recv, v_send, v_recv):
    frag = lax.axis_index("frag")
    y = lax.axis_index("dev2")
    dev = lax.axis_index("dev")
    x = dev // 2
    core = dev % 2
    partner = (frag, y, 2 * x + 1 - core)
    xnbr = [(frag, y, 2 * (1 - x) + b) for b in range(2)]
    ynbr = [(frag, 1 - y, 2 * x + b) for b in range(2)]

    small = [pltpu.make_async_copy(cot_ref, cot_v, c_sem.at[0]),
             pltpu.make_async_copy(cvt_ref, cvt_v, c_sem.at[1])]
    for copy in small:
        copy.start()

    def fetch(p, slot):
        return pltpu.make_async_copy(
            a_ref.at[p], abuf.at[slot, :, pl.ds(0, N_R)], a_sem.at[slot])

    for p in range(SLOTS):
        fetch(p, p).start()

    rest = jnp.zeros((PAIRS, 2, 2, YR - YC, 128), BF16)
    yr[:, :, :, YC:, :] = rest
    py[:, :, YC:, :] = rest[:, 0]
    rest = jnp.zeros((PAIRS, 2, 2, XR - XC, 128), BF16)
    xr[:, :, :, XC:, :] = rest
    px[:, :, XC:, :] = rest[:, 0]

    barrier = pltpu.get_barrier_semaphore()
    for peer in [partner] + xnbr + ynbr:
        pl.semaphore_signal(barrier, inc=1, device_id=peer, device_id_type=MESH)

    for s in range(SLOTS):
        abuf[s, :, N_R:, :] = jnp.zeros((N_Q, 4, N_R), BF16)
    pool[...] = jnp.zeros_like(pool)
    lhs1[...] = jnp.zeros_like(lhs1)
    w2[...] = jnp.zeros_like(w2)
    cvb[...] = jnp.zeros_like(cvb)
    cob[...] = jnp.zeros_like(cob)
    for copy in small:
        copy.wait()

    cot = cot_v[...].astype(F32)
    rep = jnp.concatenate(
        [jnp.broadcast_to(cot[j:j + 1], (8, N_R)) for j in range(N_OCC)], axis=0)
    sub = lax.broadcasted_iota(jnp.int32, (8 * N_OCC, N_R), 0) % 8
    for m in range(8):
        lhs1[m, :, :N_R] = jnp.where(sub == m, rep, 0.0).astype(BF16)

    def first(slot, k):
        sums = []
        for g in range(4):
            total = None
            for m in range(min(8, HALF - 8 * g)):
                q = 8 * g + m
                left = jnp.pad(abuf[slot, q], ((0, 0), (0, 12)))
                right = jnp.pad(abuf[slot, HALF + q], ((0, 0), (0, 12)))
                term = jnp.dot(lhs1[m], jnp.concatenate([left, right], axis=1),
                               preferred_element_type=F32)
                total = term if total is None else total + term
            sums.append(total)
        for gp in range(2):
            for j in range(N_OCC):
                for h in range(2):
                    both = jnp.concatenate(
                        [sums[2 * gp + e][8 * j:8 * j + 8, 128 * h:128 * h + 128] for e in range(2)],
                        axis=0)
                    t1[j, k * 64 + h * 32 + gp * 16:k * 64 + h * 32 + gp * 16 + 16, :] = (
                        both.astype(BF16))

    def refill(p):
        @pl.when(p + SLOTS < N_P)
        def _():
            fetch(p + SLOTS, p % SLOTS).start()

    t1[...] = jnp.zeros_like(t1)
    fetch(0, 0).wait()
    first(0, 1)
    refill(0)

    cvt = cvt_v[...].astype(F32)

    def put(xt, b, pieces):
        for kk in (0, 1):
            rows = jnp.concatenate(
                [cvt[lo:lo + n] if k == kk else jnp.zeros((n, N_R), F32) for n, lo, k in pieces]
                + [jnp.zeros((YR - YC, N_R), F32)], axis=0)
            head = jnp.concatenate([rows[:XC], jnp.zeros((XR - XC, N_R), F32)], axis=0)
            w2[xt, b * XR:(b + 1) * XR, kk * 128:kk * 128 + N_R] = head.astype(BF16)
            w2[xt, 2 * XR + b * YR:2 * XR + (b + 1) * YR, kk * 128:kk * 128 + N_R] = (
                rows[XC:].astype(BF16))

    put(0, 0, [(84, 0, 0)])
    put(0, 1, [(28, 84, 0), (56, 0, 1)])
    put(1, 0, [(56, 56, 0), (28, 0, 1)])
    put(1, 1, [(84, 28, 1)])

    cv = cvt.T
    for side in range(2):
        for h in range(2):
            lo = h * HALF
            low, high = cv[lo:lo + HALF], cv[N_Q + lo:N_Q + lo + HALF]
            part = jnp.where(y == side, low, high)
            part = jnp.concatenate([part, jnp.zeros((3, N_VIR), F32)], axis=0).astype(BF16)
            for k in range(2):
                cvb[pl.ds(side * 128 + k * 64 + h * 32, 32), k * 128:k * 128 + N_VIR] = part

    co = cot.T
    for i in range(N_OCC):
        rows = jnp.broadcast_to(co[:, i:i + 1], (N_R, 128))
        cob[i * 120 + 1:i * 120 + 1 + N_R, :] = rows
        pool[COEF + i * 120 + 1:COEF + i * 120 + 1 + N_R, :] = rows

    def second(u):
        for dx in range(2):
            xt = (x + dx) % 2
            rows = []
            for dy in range(2):
                j0 = 3 * ((y + dy) % 2) + xt
                rows.append(jnp.concatenate([t1[j0], t1[j0 + 1]], axis=1))
            half = lax.dot_general(w2[xt], jnp.concatenate(rows, axis=0), (((1,), (1,)), ((), ())),
                                   preferred_element_type=F32).astype(BF16)
            for b in range(2):
                for dy in range(2):
                    lane = slice(128 * dy, 128 * dy + 128)
                    (lx, xs)[dx][u, b, dy] = half[b * XR:(b + 1) * XR, lane]
                    (ly, ys)[dy][u, b, dx] = half[2 * XR + b * YR:2 * XR + (b + 1) * YR, lane]

    def remote(src, dst, s, r, peer):
        return pltpu.make_async_remote_copy(
            src_ref=src, dst_ref=dst, send_sem=s, recv_sem=r, device_id=peer, device_id_type=MESH)

    live_x, live = pl.ds(0, XC), pl.ds(0, YC)

    def cross_x(u, b, mark):
        return remote(xs.at[u, b, :, live_x], xr.at[u, core, :, live_x], send.at[u, b],
                      recv.at[u, mark], xnbr[b])

    def cross_y(u, b, mark):
        return remote(ys.at[u, b, :, live], yr.at[u, core, :, live], send.at[u, 2 + b],
                      recv.at[u, 2 + mark], ynbr[b])

    def pair_x(u):
        return remote(lx.at[u, 1 - core, :, live_x], px.at[u, :, live_x], send.at[u, 4],
                      recv.at[u, 4], partner)

    def pair_y(u):
        return remote(ly.at[u, 1 - core, :, live], py.at[u, :, live], send.at[u, 5],
                      recv.at[u, 5], partner)

    def send_pair(u):
        for b in range(2):
            cross_y(u, b, core).start()
            cross_x(u, b, core).start()
        pair_x(u).start()
        pair_y(u).start()

    def arrive(u):
        for b in range(2):
            cross_x(u, b, b).wait_recv()
            cross_y(u, b, b).wait_recv()
        pair_x(u).wait_recv()
        pair_y(u).wait_recv()

    def scales(u, source, table, base):
        p = source * N_P + 2 * u
        return [[jnp.broadcast_to(table[pl.ds(base + i * 120 + p + e, 1), :], (8, 128))
                 for i in range(N_OCC)] for e in range(2)]

    def gather(base, tiles, g, source, u, paced):
        for half in (0, 3):
            for lo, hi in ((0, tiles // 2), (tiles // 2, tiles)) if paced else ((0, tiles),):
                table, at = (pool, COEF) if paced else (cob, 0)
                scale = [scales(u, s, table, at) for s in source]
                for r in range(lo, hi):
                    for i in range(half, half + 3):
                        row = base + i * tiles * 8 + 8 * r
                        v = pool[row:row + 8, :]
                        for rows, sc in zip(g, scale):
                            for e in range(2):
                                v = v + sc[e][i] * rows[8 * r:8 * r + 8, 128 * e:128 * e + 128]
                        pool[row:row + 8, :] = v

    from_x = [dev, 2 * x + 1 - core, 2 * (1 - x), 2 * (1 - x) + 1]

    def third(u, paced, order=(0, 1)):
        flat = [lx[u, core], px[u], xr[u, 0], xr[u, 1]]
        ys_in = [jnp.concatenate([ly[u, core], yr[u, core]], axis=2),
                 jnp.concatenate([py[u], yr[u, 1 - core]], axis=2)]
        gx = jnp.dot(jnp.concatenate([f[d] for d in order for f in flat], axis=0), cvb[:128],
                     preferred_element_type=F32)
        gy = jnp.dot(jnp.concatenate([f[d] for d in order for f in ys_in], axis=0), cvb[...],
                     preferred_element_type=F32)
        for n, d in enumerate(order):
            for s in range(0, 4, 2):
                at = (4 * n + s) * XR
                gather(ACC_X + d * N_OCC * XR, XR // 8, [gx[at:at + XR], gx[at + XR:at + 2 * XR]],
                       from_x[s:s + 2], u, paced)
            at = 2 * n * YR
            gather(ACC_Y + d * N_OCC * YR, YR // 8, [gy[at:at + YR], gy[at + YR:at + 2 * YR]],
                   from_x[:2], u, paced)

    def stream(u):
        fetch(2 * u - 1, (2 * u - 1) % SLOTS).wait()
        fetch(2 * u, 2 * u % SLOTS).wait()

    def trip(u):
        first((2 * u - 1) % SLOTS, 0)
        first(2 * u % SLOTS, 1)
        second(u)
        send_pair(u)
        refill(2 * u - 1)
        refill(2 * u)

    pl.semaphore_wait(barrier, 5)
    second(0)
    send_pair(0)

    def early(u, carry):
        stream(u)
        trip(u)
        return carry

    def late(u, carry):
        stream(u)
        arrive(u - LAG)
        third(u - LAG, True)
        trip(u)
        return carry

    last = PAIRS - 1
    lax.fori_loop(1, LAG, early, 0)
    lax.fori_loop(LAG, last, late, 0)
    p = 2 * last - 1
    fetch(p, p % SLOTS).wait()
    first(p % SLOTS, 0)
    fetch(p + 1, (p + 1) % SLOTS).wait()
    first((p + 1) % SLOTS, 1)
    second(last)
    send_pair(last)

    def drain(n, carry):
        u = last - LAG + 2 * n
        arrive(u)
        arrive(u + 1)
        third(u, False)
        third(u + 1, False)
        return carry

    lax.fori_loop(0, LAG // 2, drain, 0)
    arrive(last)
    third(last, False, (1, 0))

    def acc_x(d, i):
        return pl.ds(ACC_X + (d * N_OCC + i) * XR, XC)

    def acc_y(d, i):
        return pl.ds(ACC_Y + (d * N_OCC + i) * YR, YC)

    def v_y(i):
        return remote(pool.at[acc_x(1, i)], vy.at[i, live_x], v_send.at[0, i], v_recv.at[0, i], (frag, 1 - y, dev))

    def v_x(i):
        return remote(pool.at[acc_y(1, i)], vx.at[i, live], v_send.at[1, i], v_recv.at[1, i],
                      (frag, y, 2 * (1 - x) + core))

    for i in range(N_OCC):
        v_y(i).start()
        v_x(i).start()
    for i in range(N_OCC):
        v_y(i).wait_recv()
        out_ref[i, :XC] = (pool[acc_x(0, i), :] + vy[i, :XC])[:, :N_VIR]
        v_x(i).wait_recv()
        out_ref[i, XC:] = (pool[acc_y(0, i), :] + vx[i, :YC])[:, :N_VIR]
    for i in range(N_OCC):
        v_y(i).wait_send()
        v_x(i).wait_send()

    def sent(u, carry):
        for b in range(2):
            cross_x(u, b, b).wait_send()
            cross_y(u, b, b).wait_send()
        pair_x(u).wait_send()
        pair_y(u).wait_send()
        return carry

    lax.fori_loop(0, PAIRS, sent, 0)


def solution(mesh):
    def local_program(ints_blk, c_occ, c_vir):
        dma = pltpu.SemaphoreType.DMA
        xb, yb = (2, XR, 128), (2, YR, 128)
        out = pl.pallas_call(
            kernel,
            out_shape=jax.ShapeDtypeStruct((N_OCC, COLS, N_VIR), F32),
            in_specs=[pl.BlockSpec(memory_space=pl.ANY)] * 3,
            out_specs=pl.BlockSpec(memory_space=pltpu.VMEM),
            scratch_shapes=[
                pltpu.VMEM((N_OCC, N_R), BF16),
                pltpu.VMEM((N_VIR, N_R), BF16),
                pltpu.VMEM((SLOTS, N_Q, 120, N_R), BF16),
                pltpu.VMEM((8, 8 * N_OCC, 120), BF16),
                pltpu.VMEM((2, 2 * (XR + YR), 256), BF16),
                pltpu.VMEM((256, 256), BF16),
                pltpu.VMEM((N_OCC * 120, 128), F32),
                pltpu.VMEM((N_OCC, 128, 128), BF16),
                pltpu.VMEM((PAIRS, 2) + xb, BF16),
                pltpu.VMEM((PAIRS, 2) + yb, BF16),
                pltpu.VMEM((PAIRS, 2) + xb, BF16),
                pltpu.VMEM((PAIRS, 2) + yb, BF16),
                pltpu.VMEM((PAIRS,) + xb, BF16),
                pltpu.VMEM((PAIRS,) + yb, BF16),
                pltpu.VMEM((PAIRS, 2) + xb, BF16),
                pltpu.VMEM((PAIRS, 2) + yb, BF16),
                pltpu.VMEM((COEF + N_OCC * 120, 128), F32),
                pltpu.VMEM((N_OCC, YR, 128), F32),
                pltpu.VMEM((N_OCC, XR, 128), F32),
                dma((SLOTS,)), dma((2,)), dma((PAIRS, 6)), dma((PAIRS, 6)),
                dma((2, N_OCC)), dma((2, N_OCC)),
            ],
            compiler_params=pltpu.CompilerParams(
                collective_id=0, has_side_effects=True,
                vmem_limit_bytes=36 * 1024 * 1024),
        )(ints_blk, pltpu.with_memory_space_constraint(c_occ.T, pltpu.HBM),
          pltpu.with_memory_space_constraint(c_vir.T, pltpu.HBM))
        return jnp.transpose(out, (0, 2, 1))

    return jax.shard_map(
        local_program,
        mesh=mesh,
        in_specs=(P(('frag', 'dev'), 'dev2', None, None), P('frag', None), P('frag', None)),
        out_specs=P(None, None, ('frag', 'dev2', 'dev')),
        check_vma=False,
    )
```

```python
import jax
import jax.numpy as jnp
from jax import lax
from jax.experimental import pallas as pl
from jax.experimental.pallas import tpu as pltpu
from jax.sharding import PartitionSpec as P

MESH = pl.DeviceIdType.MESH
F32 = jnp.float32
BF16 = jnp.bfloat16

N_P = 29
N_Q = 58
HALF = 29
N_R = 116
N_OCC = 6
N_VIR = 112
COLS = 84
XC = 42
YC = 42
XR = 48
YR = 48
SLOTS = 6
PAIRS = 15
ACC_X = 0
ACC_Y = ACC_X + 2 * N_OCC * XR
COEF = ACC_Y + 2 * N_OCC * YR
LAG = 8


def kernel(a_ref, cot_ref, cvt_ref, out_ref, cot_v, cvt_v, abuf, lhs1, w2, cvb, cob, t1,
           lx, ly, xs, ys, px, py, xr, yr, pool, vx, vy,
           a_sem, c_sem, send, recv, v_send, v_recv):
    frag = lax.axis_index("frag")
    y = lax.axis_index("dev2")
    dev = lax.axis_index("dev")
    x = dev // 2
    core = dev % 2
    partner = (frag, y, 2 * x + 1 - core)
    xnbr = [(frag, y, 2 * (1 - x) + b) for b in range(2)]
    ynbr = [(frag, 1 - y, 2 * x + b) for b in range(2)]

    small = [pltpu.make_async_copy(cot_ref, cot_v, c_sem.at[0]),
             pltpu.make_async_copy(cvt_ref, cvt_v, c_sem.at[1])]
    for copy in small:
        copy.start()

    def fetch(p, slot):
        return pltpu.make_async_copy(
            a_ref.at[p], abuf.at[slot, :, pl.ds(0, N_R)], a_sem.at[slot])

    for p in range(SLOTS):
        fetch(p, p).start()

    rest = jnp.zeros((PAIRS, 2, 2, YR - YC, 128), BF16)
    yr[:, :, :, YC:, :] = rest
    py[:, :, YC:, :] = rest[:, 0]
    rest = jnp.zeros((PAIRS, 2, 2, XR - XC, 128), BF16)
    xr[:, :, :, XC:, :] = rest
    px[:, :, XC:, :] = rest[:, 0]

    barrier = pltpu.get_barrier_semaphore()
    for peer in [partner] + xnbr + ynbr:
        pl.semaphore_signal(barrier, inc=1, device_id=peer, device_id_type=MESH)

    for s in range(SLOTS):
        abuf[s, :, N_R:, :] = jnp.zeros((N_Q, 4, N_R), BF16)
    pool[...] = jnp.zeros_like(pool)
    lhs1[...] = jnp.zeros_like(lhs1)
    w2[...] = jnp.zeros_like(w2)
    cvb[...] = jnp.zeros_like(cvb)
    cob[...] = jnp.zeros_like(cob)
    for copy in small:
        copy.wait()

    cot = cot_v[...].astype(F32)
    rep = jnp.concatenate(
        [jnp.broadcast_to(cot[j:j + 1], (8, N_R)) for j in range(N_OCC)], axis=0)
    sub = lax.broadcasted_iota(jnp.int32, (8 * N_OCC, N_R), 0) % 8
    for m in range(8):
        lhs1[m, :, :N_R] = jnp.where(sub == m, rep, 0.0).astype(BF16)

    def first(slot, par, k):
        sums = []
        for g in range(4):
            total = None
            for m in range(min(8, HALF - 8 * g)):
                q = 8 * g + m
                left = jnp.pad(abuf[slot, q], ((0, 0), (0, 12)))
                right = jnp.pad(abuf[slot, HALF + q], ((0, 0), (0, 12)))
                term = jnp.dot(lhs1[m], jnp.concatenate([left, right], axis=1),
                               preferred_element_type=F32)
                total = term if total is None else total + term
            sums.append(total)
        for gp in range(2):
            for j in range(N_OCC):
                for h in range(2):
                    both = jnp.concatenate(
                        [sums[2 * gp + e][8 * j:8 * j + 8, 128 * h:128 * h + 128] for e in range(2)],
                        axis=0)
                    t1[par, j, k * 64 + h * 32 + gp * 16:k * 64 + h * 32 + gp * 16 + 16, :] = (
                        both.astype(BF16))

    def refill(p):
        @pl.when(p + SLOTS < N_P)
        def _():
            fetch(p + SLOTS, p % SLOTS).start()

    t1[...] = jnp.zeros_like(t1)
    fetch(0, 0).wait()
    first(0, 0, 1)
    refill(0)

    cvt = cvt_v[...].astype(F32)

    def put(xt, b, pieces):
        for kk in (0, 1):
            rows = jnp.concatenate(
                [cvt[lo:lo + n] if k == kk else jnp.zeros((n, N_R), F32) for n, lo, k in pieces]
                + [jnp.zeros((YR - YC, N_R), F32)], axis=0)
            head = jnp.concatenate([rows[:XC], jnp.zeros((XR - XC, N_R), F32)], axis=0)
            w2[xt, b * XR:(b + 1) * XR, kk * 128:kk * 128 + N_R] = head.astype(BF16)
            w2[xt, 2 * XR + b * YR:2 * XR + (b + 1) * YR, kk * 128:kk * 128 + N_R] = (
                rows[XC:].astype(BF16))

    put(0, 0, [(84, 0, 0)])
    put(0, 1, [(28, 84, 0), (56, 0, 1)])
    put(1, 0, [(56, 56, 0), (28, 0, 1)])
    put(1, 1, [(84, 28, 1)])

    cv = cvt.T
    for side in range(2):
        for h in range(2):
            lo = h * HALF
            low, high = cv[lo:lo + HALF], cv[N_Q + lo:N_Q + lo + HALF]
            part = jnp.where(y == side, low, high)
            part = jnp.concatenate([part, jnp.zeros((3, N_VIR), F32)], axis=0).astype(BF16)
            for k in range(2):
                cvb[pl.ds(side * 128 + k * 64 + h * 32, 32), k * 128:k * 128 + N_VIR] = part

    co = cot.T
    for i in range(N_OCC):
        rows = jnp.broadcast_to(co[:, i:i + 1], (N_R, 128))
        cob[i * 120 + 1:i * 120 + 1 + N_R, :] = rows
        pool[COEF + i * 120 + 1:COEF + i * 120 + 1 + N_R, :] = rows

    def second(u, par):
        for dx in range(2):
            xt = (x + dx) % 2
            rows = []
            for dy in range(2):
                j0 = 3 * ((y + dy) % 2) + xt
                rows.append(jnp.concatenate([t1[par, j0], t1[par, j0 + 1]], axis=1))
            half = lax.dot_general(w2[xt], jnp.concatenate(rows, axis=0), (((1,), (1,)), ((), ())),
                                   preferred_element_type=F32).astype(BF16)
            for b in range(2):
                for dy in range(2):
                    lane = slice(128 * dy, 128 * dy + 128)
                    (lx, xs)[dx][u, b, dy] = half[b * XR:(b + 1) * XR, lane]
                    (ly, ys)[dy][u, b, dx] = half[2 * XR + b * YR:2 * XR + (b + 1) * YR, lane]

    def remote(src, dst, s, r, peer):
        return pltpu.make_async_remote_copy(
            src_ref=src, dst_ref=dst, send_sem=s, recv_sem=r, device_id=peer, device_id_type=MESH)

    live_x, live = pl.ds(0, XC), pl.ds(0, YC)

    def cross_x(u, b, mark):
        return remote(xs.at[u, b, :, live_x], xr.at[u, core, :, live_x], send.at[u, b],
                      recv.at[u, mark], xnbr[b])

    def cross_y(u, b, mark):
        return remote(ys.at[u, b, :, live], yr.at[u, core, :, live], send.at[u, 2 + b],
                      recv.at[u, 2 + mark], ynbr[b])

    def pair_x(u):
        return remote(lx.at[u, 1 - core, :, live_x], px.at[u, :, live_x], send.at[u, 4],
                      recv.at[u, 4], partner)

    def pair_y(u):
        return remote(ly.at[u, 1 - core, :, live], py.at[u, :, live], send.at[u, 5],
                      recv.at[u, 5], partner)

    def send_pair(u):
        for b in range(2):
            cross_y(u, b, core).start()
            cross_x(u, b, core).start()
        pair_x(u).start()
        pair_y(u).start()

    def arrive(u):
        for b in range(2):
            cross_x(u, b, b).wait_recv()
            cross_y(u, b, b).wait_recv()
        pair_x(u).wait_recv()
        pair_y(u).wait_recv()

    def scales(u, source, table, base):
        p = source * N_P + 2 * u
        return [[jnp.broadcast_to(table[pl.ds(base + i * 120 + p + e, 1), :], (8, 128))
                 for i in range(N_OCC)] for e in range(2)]

    def gather(base, tiles, g, source, u, paced):
        for half in (0, 3):
            for lo, hi in ((0, tiles // 2), (tiles // 2, tiles)) if paced else ((0, tiles),):
                table, at = (pool, COEF) if paced else (cob, 0)
                scale = [scales(u, s, table, at) for s in source]
                for r in range(lo, hi):
                    for i in range(half, half + 3):
                        row = base + i * tiles * 8 + 8 * r
                        v = pool[row:row + 8, :]
                        for rows, sc in zip(g, scale):
                            for e in range(2):
                                v = v + sc[e][i] * rows[8 * r:8 * r + 8, 128 * e:128 * e + 128]
                        pool[row:row + 8, :] = v

    from_x = [dev, 2 * x + 1 - core, 2 * (1 - x), 2 * (1 - x) + 1]

    def third(u, paced, order=(0, 1), between=None):
        flat = [lx[u, core], px[u], xr[u, 0], xr[u, 1]]
        ys_in = [jnp.concatenate([ly[u, core], yr[u, core]], axis=2),
                 jnp.concatenate([py[u], yr[u, 1 - core]], axis=2)]
        gx = jnp.dot(jnp.concatenate([f[d] for d in order for f in flat], axis=0), cvb[:128],
                     preferred_element_type=F32)
        gy = jnp.dot(jnp.concatenate([f[d] for d in order for f in ys_in], axis=0), cvb[...],
                     preferred_element_type=F32)
        for n, d in enumerate(order):
            for s in range(0, 4, 2):
                at = (4 * n + s) * XR
                gather(ACC_X + d * N_OCC * XR, XR // 8, [gx[at:at + XR], gx[at + XR:at + 2 * XR]],
                       from_x[s:s + 2], u, paced)
            at = 2 * n * YR
            gather(ACC_Y + d * N_OCC * YR, YR // 8, [gy[at:at + YR], gy[at + YR:at + 2 * YR]],
                   from_x[:2], u, paced)
            if n == 0 and between is not None:
                between()


    def stream(u):
        fetch(2 * u - 1, (2 * u - 1) % SLOTS).wait()
        fetch(2 * u, 2 * u % SLOTS).wait()

    def trip(u, before=True):
        first((2 * u - 1) % SLOTS, u % 2, 0)
        first(2 * u % SLOTS, u % 2, 1)
        if before:
            send_pair(u - 1)
        refill(2 * u - 1)
        refill(2 * u)

    pl.semaphore_wait(barrier, 5)
    second(0, 0)
    send_pair(0)
    stream(1)
    trip(1, False)

    def early(u, carry):
        stream(u)
        second(u - 1, (u + 1) % 2)
        trip(u)
        return carry

    def late(u, carry):
        stream(u)
        arrive(u - LAG)
        third(u - LAG, True)
        second(u - 1, (u + 1) % 2)
        trip(u)
        return carry

    last = PAIRS - 1
    lax.fori_loop(2, LAG, early, 0)
    lax.fori_loop(LAG, last, late, 0)
    second(last - 1, (last - 1) % 2)
    send_pair(last - 1)
    p = 2 * last - 1
    fetch(p, p % SLOTS).wait()
    first(p % SLOTS, last % 2, 0)
    fetch(p + 1, (p + 1) % SLOTS).wait()
    first((p + 1) % SLOTS, last % 2, 1)
    second(last, last % 2)
    send_pair(last)

    def drain(n, carry):
        u = last - LAG + 2 * n
        arrive(u)
        arrive(u + 1)
        third(u, False)
        third(u + 1, False)
        return carry

    lax.fori_loop(0, LAG // 2, drain, 0)
    def acc_x(d, i):
        return pl.ds(ACC_X + (d * N_OCC + i) * XR, XC)

    def acc_y(d, i):
        return pl.ds(ACC_Y + (d * N_OCC + i) * YR, YC)

    def v_y(i):
        return remote(pool.at[acc_x(1, i)], vy.at[i, live_x], v_send.at[0, i], v_recv.at[0, i], (frag, 1 - y, dev))

    def v_x(i):
        return remote(pool.at[acc_y(1, i)], vx.at[i, live], v_send.at[1, i], v_recv.at[1, i],
                      (frag, y, 2 * (1 - x) + core))

    def share():
        for i in range(N_OCC):
            v_y(i).start()
            v_x(i).start()

    arrive(last)
    third(last, False, (1, 0), share)
    for i in range(N_OCC):
        v_y(i).wait_recv()
        out_ref[i, :XC] = (pool[acc_x(0, i), :] + vy[i, :XC])[:, :N_VIR]
        v_x(i).wait_recv()
        out_ref[i, XC:] = (pool[acc_y(0, i), :] + vx[i, :YC])[:, :N_VIR]
    for i in range(N_OCC):
        v_y(i).wait_send()
        v_x(i).wait_send()

    def sent(u, carry):
        for b in range(2):
            cross_x(u, b, b).wait_send()
            cross_y(u, b, b).wait_send()
        pair_x(u).wait_send()
        pair_y(u).wait_send()
        return carry

    lax.fori_loop(0, PAIRS, sent, 0)


def solution(mesh):
    def local_program(ints_blk, c_occ, c_vir):
        dma = pltpu.SemaphoreType.DMA
        xb, yb = (2, XR, 128), (2, YR, 128)
        out = pl.pallas_call(
            kernel,
            out_shape=jax.ShapeDtypeStruct((N_OCC, COLS, N_VIR), F32),
            in_specs=[pl.BlockSpec(memory_space=pl.ANY)] * 3,
            out_specs=pl.BlockSpec(memory_space=pltpu.VMEM),
            scratch_shapes=[
                pltpu.VMEM((N_OCC, N_R), BF16),
                pltpu.VMEM((N_VIR, N_R), BF16),
                pltpu.VMEM((SLOTS, N_Q, 120, N_R), BF16),
                pltpu.VMEM((8, 8 * N_OCC, 120), BF16),
                pltpu.VMEM((2, 2 * (XR + YR), 256), BF16),
                pltpu.VMEM((256, 256), BF16),
                pltpu.VMEM((N_OCC * 120, 128), F32),
                pltpu.VMEM((2, N_OCC, 128, 128), BF16),
                pltpu.VMEM((PAIRS, 2) + xb, BF16),
                pltpu.VMEM((PAIRS, 2) + yb, BF16),
                pltpu.VMEM((PAIRS, 2) + xb, BF16),
                pltpu.VMEM((PAIRS, 2) + yb, BF16),
                pltpu.VMEM((PAIRS,) + xb, BF16),
                pltpu.VMEM((PAIRS,) + yb, BF16),
                pltpu.VMEM((PAIRS, 2) + xb, BF16),
                pltpu.VMEM((PAIRS, 2) + yb, BF16),
                pltpu.VMEM((COEF + N_OCC * 120, 128), F32),
                pltpu.VMEM((N_OCC, YR, 128), F32),
                pltpu.VMEM((N_OCC, XR, 128), F32),
                dma((SLOTS,)), dma((2,)), dma((PAIRS, 6)), dma((PAIRS, 6)),
                dma((2, N_OCC)), dma((2, N_OCC)),
            ],
            compiler_params=pltpu.CompilerParams(
                collective_id=0, has_side_effects=True,
                vmem_limit_bytes=36 * 1024 * 1024),
        )(ints_blk, pltpu.with_memory_space_constraint(c_occ.T, pltpu.HBM),
          pltpu.with_memory_space_constraint(c_vir.T, pltpu.HBM))
        return jnp.transpose(out, (0, 2, 1))

    return jax.shard_map(
        local_program,
        mesh=mesh,
        in_specs=(P(('frag', 'dev'), 'dev2', None, None), P('frag', None), P('frag', None)),
        out_specs=P(None, None, ('frag', 'dev2', 'dev')),
        check_vma=False,
    )
```

```python
import jax
import jax.numpy as jnp
from jax import lax
from jax.experimental import pallas as pl
from jax.experimental.pallas import tpu as pltpu
from jax.sharding import PartitionSpec as P

MESH = pl.DeviceIdType.MESH
F32 = jnp.float32
BF16 = jnp.bfloat16

N_P = 29
N_Q = 58
HALF = 29
N_R = 116
N_OCC = 6
N_VIR = 112
COLS = 84
XC = 42
YC = 42
XR = 48
YR = 48
SLOTS = 6
PAIRS = 15
ACC_X = 0
ACC_Y = ACC_X + 2 * N_OCC * XR
COEF = ACC_Y + 2 * N_OCC * YR
LAG = 10


def kernel(a_ref, cot_ref, cvt_ref, out_ref, cot_v, cvt_v, abuf, lhs1, w2, cvb, cob, t1,
           lx, ly, xs, ys, px, py, xr, yr, pool, vx, vy,
           a_sem, c_sem, send, recv, v_send, v_recv):
    frag = lax.axis_index("frag")
    y = lax.axis_index("dev2")
    dev = lax.axis_index("dev")
    x = dev // 2
    core = dev % 2
    partner = (frag, y, 2 * x + 1 - core)
    xnbr = [(frag, y, 2 * (1 - x) + b) for b in range(2)]
    ynbr = [(frag, 1 - y, 2 * x + b) for b in range(2)]

    small = [pltpu.make_async_copy(cot_ref, cot_v, c_sem.at[0]),
             pltpu.make_async_copy(cvt_ref, cvt_v, c_sem.at[1])]
    for copy in small:
        copy.start()

    def fetch(p, slot):
        return pltpu.make_async_copy(
            a_ref.at[p], abuf.at[slot, :, pl.ds(0, N_R)], a_sem.at[slot])

    for p in range(SLOTS):
        fetch(p, p).start()

    rest = jnp.zeros((PAIRS, 2, 2, YR - YC, 128), BF16)
    yr[:, :, :, YC:, :] = rest
    py[:, :, YC:, :] = rest[:, 0]
    rest = jnp.zeros((PAIRS, 2, 2, XR - XC, 128), BF16)
    xr[:, :, :, XC:, :] = rest
    px[:, :, XC:, :] = rest[:, 0]

    barrier = pltpu.get_barrier_semaphore()
    for peer in [partner] + xnbr + ynbr:
        pl.semaphore_signal(barrier, inc=1, device_id=peer, device_id_type=MESH)

    for s in range(SLOTS):
        abuf[s, :, N_R:, :] = jnp.zeros((N_Q, 4, N_R), BF16)
    pool[...] = jnp.zeros_like(pool)
    lhs1[...] = jnp.zeros_like(lhs1)
    w2[...] = jnp.zeros_like(w2)
    cvb[...] = jnp.zeros_like(cvb)
    cob[...] = jnp.zeros_like(cob)
    for copy in small:
        copy.wait()

    cot = cot_v[...].astype(F32)
    rep = jnp.concatenate(
        [jnp.broadcast_to(cot[j:j + 1], (8, N_R)) for j in range(N_OCC)], axis=0)
    sub = lax.broadcasted_iota(jnp.int32, (8 * N_OCC, N_R), 0) % 8
    for m in range(8):
        lhs1[m, :, :N_R] = jnp.where(sub == m, rep, 0.0).astype(BF16)

    def first(slot, par, k):
        sums = []
        for g in range(4):
            total = None
            for m in range(min(8, HALF - 8 * g)):
                q = 8 * g + m
                left = jnp.pad(abuf[slot, q], ((0, 0), (0, 12)))
                right = jnp.pad(abuf[slot, HALF + q], ((0, 0), (0, 12)))
                term = jnp.dot(lhs1[m], jnp.concatenate([left, right], axis=1),
                               preferred_element_type=F32)
                total = term if total is None else total + term
            sums.append(total)
        for gp in range(2):
            for j in range(N_OCC):
                for h in range(2):
                    both = jnp.concatenate(
                        [sums[2 * gp + e][8 * j:8 * j + 8, 128 * h:128 * h + 128] for e in range(2)],
                        axis=0)
                    t1[par, j, k * 64 + h * 32 + gp * 16:k * 64 + h * 32 + gp * 16 + 16, :] = (
                        both.astype(BF16))

    def refill(p):
        @pl.when(p + SLOTS < N_P)
        def _():
            fetch(p + SLOTS, p % SLOTS).start()

    t1[...] = jnp.zeros_like(t1)
    fetch(0, 0).wait()
    first(0, 0, 1)
    refill(0)

    cvt = cvt_v[...].astype(F32)

    def put(xt, b, pieces):
        for kk in (0, 1):
            rows = jnp.concatenate(
                [cvt[lo:lo + n] if k == kk else jnp.zeros((n, N_R), F32) for n, lo, k in pieces]
                + [jnp.zeros((YR - YC, N_R), F32)], axis=0)
            head = jnp.concatenate([rows[:XC], jnp.zeros((XR - XC, N_R), F32)], axis=0)
            w2[xt, b * XR:(b + 1) * XR, kk * 128:kk * 128 + N_R] = head.astype(BF16)
            w2[xt, 2 * XR + b * YR:2 * XR + (b + 1) * YR, kk * 128:kk * 128 + N_R] = (
                rows[XC:].astype(BF16))

    put(0, 0, [(84, 0, 0)])
    put(0, 1, [(28, 84, 0), (56, 0, 1)])
    put(1, 0, [(56, 56, 0), (28, 0, 1)])
    put(1, 1, [(84, 28, 1)])

    cv = cvt.T
    for side in range(2):
        for h in range(2):
            lo = h * HALF
            low, high = cv[lo:lo + HALF], cv[N_Q + lo:N_Q + lo + HALF]
            part = jnp.where(y == side, low, high)
            part = jnp.concatenate([part, jnp.zeros((3, N_VIR), F32)], axis=0).astype(BF16)
            for k in range(2):
                cvb[pl.ds(side * 128 + k * 64 + h * 32, 32), k * 128:k * 128 + N_VIR] = part

    co = cot.T
    for i in range(N_OCC):
        rows = jnp.broadcast_to(co[:, i:i + 1], (N_R, 128))
        cob[i * 120 + 1:i * 120 + 1 + N_R, :] = rows
        pool[COEF + i * 120 + 1:COEF + i * 120 + 1 + N_R, :] = rows

    def second(u, par):
        for dx in range(2):
            xt = (x + dx) % 2
            rows = []
            for dy in range(2):
                j0 = 3 * ((y + dy) % 2) + xt
                rows.append(jnp.concatenate([t1[par, j0], t1[par, j0 + 1]], axis=1))
            half = lax.dot_general(w2[xt], jnp.concatenate(rows, axis=0), (((1,), (1,)), ((), ())),
                                   preferred_element_type=F32).astype(BF16)
            for b in range(2):
                for dy in range(2):
                    lane = slice(128 * dy, 128 * dy + 128)
                    (lx, xs)[dx][u, b, dy] = half[b * XR:(b + 1) * XR, lane]
                    (ly, ys)[dy][u, b, dx] = half[2 * XR + b * YR:2 * XR + (b + 1) * YR, lane]

    def remote(src, dst, s, r, peer):
        return pltpu.make_async_remote_copy(
            src_ref=src, dst_ref=dst, send_sem=s, recv_sem=r, device_id=peer, device_id_type=MESH)

    live_x, live = pl.ds(0, XC), pl.ds(0, YC)

    def cross_x(u, b, mark):
        return remote(xs.at[u, b, :, live_x], xr.at[u, core, :, live_x], send.at[u, b],
                      recv.at[u, mark], xnbr[b])

    def cross_y(u, b, mark):
        return remote(ys.at[u, b, :, live], yr.at[u, core, :, live], send.at[u, 2 + b],
                      recv.at[u, 2 + mark], ynbr[b])

    def pair_x(u):
        return remote(lx.at[u, 1 - core, :, live_x], px.at[u, :, live_x], send.at[u, 4],
                      recv.at[u, 4], partner)

    def pair_y(u):
        return remote(ly.at[u, 1 - core, :, live], py.at[u, :, live], send.at[u, 5],
                      recv.at[u, 5], partner)

    def send_pair(u):
        for b in range(2):
            cross_y(u, b, core).start()
            cross_x(u, b, core).start()
        pair_x(u).start()
        pair_y(u).start()

    def arrive(u):
        for b in range(2):
            cross_x(u, b, b).wait_recv()
            cross_y(u, b, b).wait_recv()
        pair_x(u).wait_recv()
        pair_y(u).wait_recv()

    def scales(u, source, table, base):
        p = source * N_P + 2 * u
        return [[jnp.broadcast_to(table[pl.ds(base + i * 120 + p + e, 1), :], (8, 128))
                 for i in range(N_OCC)] for e in range(2)]

    def gather(base, tiles, g, source, u, half, paced):
        for lo, hi in ((0, tiles // 2), (tiles // 2, tiles)) if paced else ((0, tiles),):
            table, at = (pool, COEF) if paced else (cob, 0)
            scale = [scales(u, s, table, at) for s in source]
            for r in range(lo, hi):
                for i in range(half, half + 3):
                    row = base + i * tiles * 8 + 8 * r
                    v = pool[row:row + 8, :]
                    for rows, sc in zip(g, scale):
                        for e in range(2):
                            v = v + sc[e][i] * rows[8 * r:8 * r + 8, 128 * e:128 * e + 128]
                    pool[row:row + 8, :] = v

    from_x = [dev, 2 * x + 1 - core, 2 * (1 - x), 2 * (1 - x) + 1]

    def third(u, paced, order=(0, 1), between=None):
        flat = [lx[u, core], px[u], xr[u, 0], xr[u, 1]]
        ys_in = [jnp.concatenate([ly[u, core], yr[u, core]], axis=2),
                 jnp.concatenate([py[u], yr[u, 1 - core]], axis=2)]
        gx = jnp.dot(jnp.concatenate([f[d] for d in order for f in flat], axis=0), cvb[:128],
                     preferred_element_type=F32)
        gy = jnp.dot(jnp.concatenate([f[d] for d in order for f in ys_in], axis=0), cvb[...],
                     preferred_element_type=F32)
        for n, d in enumerate(order):
            for half in (0, 3):
                for s in range(0, 4, 2):
                    at = (len(flat) * n + s) * XR
                    gather(ACC_X + d * N_OCC * XR, XR // 8,
                           [gx[at:at + XR], gx[at + XR:at + 2 * XR]], from_x[s:s + 2], u, half, paced)
                at = 2 * n * YR
                gather(ACC_Y + d * N_OCC * YR, YR // 8,
                       [gy[at:at + YR], gy[at + YR:at + 2 * YR]], from_x[:2], u, half, paced)
                if between is not None:
                    between(half)


    def stream(u):
        fetch(2 * u - 1, (2 * u - 1) % SLOTS).wait()
        fetch(2 * u, 2 * u % SLOTS).wait()

    def trip(u, before=True):
        first((2 * u - 1) % SLOTS, u % 2, 0)
        first(2 * u % SLOTS, u % 2, 1)
        if before:
            send_pair(u - 1)
        refill(2 * u - 1)
        refill(2 * u)

    pl.semaphore_wait(barrier, 5)
    second(0, 0)
    send_pair(0)
    stream(1)
    trip(1, False)

    def early(u, carry):
        stream(u)
        second(u - 1, (u + 1) % 2)
        trip(u)
        return carry

    def late(u, carry):
        stream(u)
        arrive(u - LAG)
        third(u - LAG, True)
        second(u - 1, (u + 1) % 2)
        trip(u)
        return carry

    last = PAIRS - 1
    lax.fori_loop(2, LAG, early, 0)
    lax.fori_loop(LAG, last, late, 0)
    second(last - 1, (last - 1) % 2)
    send_pair(last - 1)
    p = 2 * last - 1
    stream(last)
    first(p % SLOTS, last % 2, 0)
    first((p + 1) % SLOTS, last % 2, 1)
    second(last, last % 2)
    send_pair(last)

    def drain(n, carry):
        u = last - LAG + 2 * n
        arrive(u)
        arrive(u + 1)
        third(u, False)
        third(u + 1, False)
        return carry

    lax.fori_loop(0, LAG // 2, drain, 0)
    def acc_x(d, i):
        return pl.ds(ACC_X + (d * N_OCC + i) * XR, XC)

    def acc_y(d, i):
        return pl.ds(ACC_Y + (d * N_OCC + i) * YR, YC)

    def v_y(i):
        return remote(pool.at[acc_x(1, i)], vy.at[i, live_x], v_send.at[0, i], v_recv.at[0, i], (frag, 1 - y, dev))

    def v_x(i):
        return remote(pool.at[acc_y(1, i)], vx.at[i, live], v_send.at[1, i], v_recv.at[1, i],
                      (frag, y, 2 * (1 - x) + core))

    def share(half):
        for i in range(half, half + 3):
            v_y(i).start()
            v_x(i).start()

    arrive(last)
    third(last, False, (1,), share)
    third(last, False, (0,))

    def sent(u, carry):
        for b in range(2):
            cross_x(u, b, b).wait_send()
            cross_y(u, b, b).wait_send()
        pair_x(u).wait_send()
        pair_y(u).wait_send()
        return carry

    lax.fori_loop(0, PAIRS, sent, 0)

    for i in range(N_OCC):
        v_y(i).wait_recv()
        out_ref[i, :XC] = (pool[acc_x(0, i), :] + vy[i, :XC])[:, :N_VIR]
        v_x(i).wait_recv()
        out_ref[i, XC:] = (pool[acc_y(0, i), :] + vx[i, :YC])[:, :N_VIR]
    for i in range(N_OCC):
        v_y(i).wait_send()
        v_x(i).wait_send()


def solution(mesh):
    def local_program(ints_blk, c_occ, c_vir):
        dma = pltpu.SemaphoreType.DMA
        xb, yb = (2, XR, 128), (2, YR, 128)
        out = pl.pallas_call(
            kernel,
            out_shape=jax.ShapeDtypeStruct((N_OCC, COLS, N_VIR), F32),
            in_specs=[pl.BlockSpec(memory_space=pl.ANY)] * 3,
            out_specs=pl.BlockSpec(memory_space=pltpu.VMEM),
            scratch_shapes=[
                pltpu.VMEM((N_OCC, N_R), BF16),
                pltpu.VMEM((N_VIR, N_R), BF16),
                pltpu.VMEM((SLOTS, N_Q, 120, N_R), BF16),
                pltpu.VMEM((8, 8 * N_OCC, 120), BF16),
                pltpu.VMEM((2, 2 * (XR + YR), 256), BF16),
                pltpu.VMEM((256, 256), BF16),
                pltpu.VMEM((N_OCC * 120, 128), F32),
                pltpu.VMEM((2, N_OCC, 128, 128), BF16),
                pltpu.VMEM((PAIRS, 2) + xb, BF16),
                pltpu.VMEM((PAIRS, 2) + yb, BF16),
                pltpu.VMEM((PAIRS, 2) + xb, BF16),
                pltpu.VMEM((PAIRS, 2) + yb, BF16),
                pltpu.VMEM((PAIRS,) + xb, BF16),
                pltpu.VMEM((PAIRS,) + yb, BF16),
                pltpu.VMEM((PAIRS, 2) + xb, BF16),
                pltpu.VMEM((PAIRS, 2) + yb, BF16),
                pltpu.VMEM((COEF + N_OCC * 120, 128), F32),
                pltpu.VMEM((N_OCC, YR, 128), F32),
                pltpu.VMEM((N_OCC, XR, 128), F32),
                dma((SLOTS,)), dma((2,)), dma((PAIRS, 6)), dma((PAIRS, 6)),
                dma((2, N_OCC)), dma((2, N_OCC)),
            ],
            compiler_params=pltpu.CompilerParams(
                collective_id=0, has_side_effects=True,
                vmem_limit_bytes=36 * 1024 * 1024),
        )(ints_blk, pltpu.with_memory_space_constraint(c_occ.T, pltpu.HBM),
          pltpu.with_memory_space_constraint(c_vir.T, pltpu.HBM))
        return jnp.transpose(out, (0, 2, 1))

    return jax.shard_map(
        local_program,
        mesh=mesh,
        in_specs=(P(('frag', 'dev'), 'dev2', None, None), P('frag', None), P('frag', None)),
        out_specs=P(None, None, ('frag', 'dev2', 'dev')),
        check_vma=False,
    )
```

```python
import jax
import jax.numpy as jnp
from jax import lax
from jax.experimental import pallas as pl
from jax.experimental.pallas import tpu as pltpu
from jax.sharding import PartitionSpec as P

MESH = pl.DeviceIdType.MESH
F32 = jnp.float32
BF16 = jnp.bfloat16

N_P = 29
N_Q = 58
HALF = 29
N_R = 116
N_OCC = 6
N_VIR = 112
COLS = 84
XC = 42
YC = 42
XR = 48
YR = 48
SLOTS = 6
PAIRS = 15
ACC_X = 0
ACC_Y = ACC_X + 2 * N_OCC * XR
COEF = ACC_Y + 2 * N_OCC * YR
LAG = 10


def kernel(a_ref, cot_ref, cvt_ref, out_ref, cot_v, cvt_v, abuf, lhs1, w2, cvb, cob, t1,
           lx, ly, xs, ys, px, py, xr, yr, pool, vx, vy,
           a_sem, c_sem, send, recv, v_send, v_recv):
    frag = lax.axis_index("frag")
    y = lax.axis_index("dev2")
    dev = lax.axis_index("dev")
    x = dev // 2
    core = dev % 2
    partner = (frag, y, 2 * x + 1 - core)
    xnbr = [(frag, y, 2 * (1 - x) + b) for b in range(2)]
    ynbr = [(frag, 1 - y, 2 * x + b) for b in range(2)]

    small = [pltpu.make_async_copy(cot_ref, cot_v, c_sem.at[0]),
             pltpu.make_async_copy(cvt_ref, cvt_v, c_sem.at[1])]
    for copy in small:
        copy.start()

    def fetch(p, slot):
        return pltpu.make_async_copy(
            a_ref.at[p], abuf.at[slot, :, pl.ds(0, N_R)], a_sem.at[slot])

    for p in range(SLOTS):
        fetch(p, p).start()

    rest = jnp.zeros((PAIRS, 2, 2, YR - YC, 128), BF16)
    yr[:, :, :, YC:, :] = rest
    py[:, :, YC:, :] = rest[:, 0]
    rest = jnp.zeros((PAIRS, 2, 2, XR - XC, 128), BF16)
    xr[:, :, :, XC:, :] = rest
    px[:, :, XC:, :] = rest[:, 0]

    barrier = pltpu.get_barrier_semaphore()
    for peer in [partner] + xnbr + ynbr:
        pl.semaphore_signal(barrier, inc=1, device_id=peer, device_id_type=MESH)

    for s in range(SLOTS):
        abuf[s, :, N_R:, :] = jnp.zeros((N_Q, 4, N_R), BF16)
    pool[...] = jnp.zeros_like(pool)
    lhs1[...] = jnp.zeros_like(lhs1)
    w2[...] = jnp.zeros_like(w2)
    cvb[...] = jnp.zeros_like(cvb)
    cob[...] = jnp.zeros_like(cob)
    for copy in small:
        copy.wait()

    cot = cot_v[...].astype(F32)
    rep = jnp.concatenate(
        [jnp.broadcast_to(cot[j:j + 1], (8, N_R)) for j in range(N_OCC)], axis=0)
    sub = lax.broadcasted_iota(jnp.int32, (8 * N_OCC, N_R), 0) % 8
    for m in range(8):
        lhs1[m, :, :N_R] = jnp.where(sub == m, rep, 0.0).astype(BF16)

    def first(slot, par, k):
        sums = []
        for g in range(4):
            total = None
            for m in range(min(8, HALF - 8 * g)):
                q = 8 * g + m
                left = jnp.pad(abuf[slot, q], ((0, 0), (0, 12)))
                right = jnp.pad(abuf[slot, HALF + q], ((0, 0), (0, 12)))
                term = jnp.dot(lhs1[m], jnp.concatenate([left, right], axis=1),
                               preferred_element_type=F32)
                total = term if total is None else total + term
            sums.append(total)
        for gp in range(2):
            for j in range(N_OCC):
                for h in range(2):
                    both = jnp.concatenate(
                        [sums[2 * gp + e][8 * j:8 * j + 8, 128 * h:128 * h + 128] for e in range(2)],
                        axis=0)
                    t1[par, j, k * 64 + h * 32 + gp * 16:k * 64 + h * 32 + gp * 16 + 16, :] = (
                        both.astype(BF16))

    def refill(p):
        @pl.when(p + SLOTS < N_P)
        def _():
            fetch(p + SLOTS, p % SLOTS).start()

    t1[...] = jnp.zeros_like(t1)
    fetch(0, 0).wait()
    first(0, 0, 1)
    refill(0)

    cvt = cvt_v[...].astype(F32)

    def put(xt, b, pieces):
        for kk in (0, 1):
            rows = jnp.concatenate(
                [cvt[lo:lo + n] if k == kk else jnp.zeros((n, N_R), F32) for n, lo, k in pieces]
                + [jnp.zeros((YR - YC, N_R), F32)], axis=0)
            head = jnp.concatenate([rows[:XC], jnp.zeros((XR - XC, N_R), F32)], axis=0)
            w2[xt, b * XR:(b + 1) * XR, kk * 128:kk * 128 + N_R] = head.astype(BF16)
            w2[xt, 2 * XR + b * YR:2 * XR + (b + 1) * YR, kk * 128:kk * 128 + N_R] = (
                rows[XC:].astype(BF16))

    put(0, 0, [(84, 0, 0)])
    put(0, 1, [(28, 84, 0), (56, 0, 1)])
    put(1, 0, [(56, 56, 0), (28, 0, 1)])
    put(1, 1, [(84, 28, 1)])

    cv = cvt.T
    for side in range(2):
        for h in range(2):
            lo = h * HALF
            low, high = cv[lo:lo + HALF], cv[N_Q + lo:N_Q + lo + HALF]
            part = jnp.where(y == side, low, high)
            part = jnp.concatenate([part, jnp.zeros((3, N_VIR), F32)], axis=0).astype(BF16)
            for k in range(2):
                cvb[pl.ds(side * 128 + k * 64 + h * 32, 32), k * 128:k * 128 + N_VIR] = part

    co = cot.T
    for i in range(N_OCC):
        rows = jnp.broadcast_to(co[:, i:i + 1], (N_R, 128))
        cob[i * 120 + 1:i * 120 + 1 + N_R, :] = rows
        pool[COEF + i * 120 + 1:COEF + i * 120 + 1 + N_R, :] = rows

    def second(u, par):
        for dx in range(2):
            xt = (x + dx) % 2
            rows = []
            for dy in range(2):
                j0 = 3 * ((y + dy) % 2) + xt
                rows.append(jnp.concatenate([t1[par, j0], t1[par, j0 + 1]], axis=1))
            half = lax.dot_general(w2[xt], jnp.concatenate(rows, axis=0), (((1,), (1,)), ((), ())),
                                   preferred_element_type=F32).astype(BF16)
            for b in range(2):
                for dy in range(2):
                    lane = slice(128 * dy, 128 * dy + 128)
                    (lx, xs)[dx][u, b, dy] = half[b * XR:(b + 1) * XR, lane]
                    (ly, ys)[dy][u, b, dx] = half[2 * XR + b * YR:2 * XR + (b + 1) * YR, lane]

    def remote(src, dst, s, r, peer):
        return pltpu.make_async_remote_copy(
            src_ref=src, dst_ref=dst, send_sem=s, recv_sem=r, device_id=peer, device_id_type=MESH)

    live_x, live = pl.ds(0, XC), pl.ds(0, YC)

    def cross_x(u, b, mark):
        return remote(xs.at[u, b, :, live_x], xr.at[u, core, :, live_x], send.at[u, b],
                      recv.at[u, mark], xnbr[b])

    def cross_y(u, b, mark):
        return remote(ys.at[u, b, :, live], yr.at[u, core, :, live], send.at[u, 2 + b],
                      recv.at[u, 2 + mark], ynbr[b])

    def pair_x(u):
        return remote(lx.at[u, 1 - core, :, live_x], px.at[u, :, live_x], send.at[u, 4],
                      recv.at[u, 4], partner)

    def pair_y(u):
        return remote(ly.at[u, 1 - core, :, live], py.at[u, :, live], send.at[u, 5],
                      recv.at[u, 5], partner)

    def send_pair(u):
        for b in range(2):
            cross_y(u, b, core).start()
            cross_x(u, b, core).start()
        pair_x(u).start()
        pair_y(u).start()

    def arrive(u):
        for b in range(2):
            cross_x(u, b, b).wait_recv()
            cross_y(u, b, b).wait_recv()
        pair_x(u).wait_recv()
        pair_y(u).wait_recv()

    def scales(u, source, table, base):
        p = source * N_P + 2 * u
        return [[jnp.broadcast_to(table[pl.ds(base + i * 120 + p + e, 1), :], (8, 128))
                 for i in range(N_OCC)] for e in range(2)]

    def gather(base, tiles, g, source, u, half, paced):
        for lo, hi in ((0, tiles // 2), (tiles // 2, tiles)) if paced else ((0, tiles),):
            table, at = (pool, COEF) if paced else (cob, 0)
            scale = [scales(u, s, table, at) for s in source]
            for r in range(lo, hi):
                for i in range(half, half + 3):
                    row = base + i * tiles * 8 + 8 * r
                    v = pool[row:row + 8, :]
                    for rows, sc in zip(g, scale):
                        for e in range(2):
                            v = v + sc[e][i] * rows[8 * r:8 * r + 8, 128 * e:128 * e + 128]
                    pool[row:row + 8, :] = v

    from_x = [dev, 2 * x + 1 - core, 2 * (1 - x), 2 * (1 - x) + 1]

    def third(u, paced, order=(0, 1), between=None):
        flat = [lx[u, core], px[u], xr[u, 0], xr[u, 1]]
        ys_in = [jnp.concatenate([ly[u, core], yr[u, core]], axis=2),
                 jnp.concatenate([py[u], yr[u, 1 - core]], axis=2)]
        gx = jnp.dot(jnp.concatenate([f[d] for d in order for f in flat], axis=0), cvb[:128],
                     preferred_element_type=F32)
        gy = jnp.dot(jnp.concatenate([f[d] for d in order for f in ys_in], axis=0), cvb[...],
                     preferred_element_type=F32)
        for n, d in enumerate(order):
            for half in (0, 3):
                for s in range(0, 4, 2):
                    at = (len(flat) * n + s) * XR
                    gather(ACC_X + d * N_OCC * XR, XR // 8,
                           [gx[at:at + XR], gx[at + XR:at + 2 * XR]], from_x[s:s + 2], u, half, paced)
                at = 2 * n * YR
                gather(ACC_Y + d * N_OCC * YR, YR // 8,
                       [gy[at:at + YR], gy[at + YR:at + 2 * YR]], from_x[:2], u, half, paced)
                if between is not None:
                    between(half)


    def stream(u):
        fetch(2 * u - 1, (2 * u - 1) % SLOTS).wait()
        fetch(2 * u, 2 * u % SLOTS).wait()

    def trip(u, before=True):
        first((2 * u - 1) % SLOTS, u % 2, 0)
        first(2 * u % SLOTS, u % 2, 1)
        if before:
            send_pair(u - 1)
        refill(2 * u - 1)
        refill(2 * u)

    pl.semaphore_wait(barrier, 5)
    second(0, 0)
    send_pair(0)

    def early(u, carry):
        stream(u)
        first((2 * u - 1) % SLOTS, u % 2, 0)
        first(2 * u % SLOTS, u % 2, 1)
        second(u, u % 2)
        send_pair(u)
        refill(2 * u - 1)
        refill(2 * u)
        return carry

    def late(u, carry):
        stream(u)
        arrive(u - LAG)
        third(u - LAG, True)
        second(u - 1, (u + 1) % 2)
        trip(u)
        return carry

    last = PAIRS - 1
    lax.fori_loop(1, LAG, early, 0)
    stream(LAG)
    arrive(0)
    third(0, True)
    trip(LAG, False)
    lax.fori_loop(LAG + 1, last, late, 0)
    second(last - 1, (last - 1) % 2)
    send_pair(last - 1)
    p = 2 * last - 1
    stream(last)
    first(p % SLOTS, last % 2, 0)
    first((p + 1) % SLOTS, last % 2, 1)
    second(last, last % 2)
    send_pair(last)

    def drain(n, carry):
        u = last - LAG + 2 * n
        arrive(u)
        arrive(u + 1)
        third(u, False)
        third(u + 1, False)
        return carry

    lax.fori_loop(0, LAG // 2, drain, 0)
    def acc_x(d, i):
        return pl.ds(ACC_X + (d * N_OCC + i) * XR, XC)

    def acc_y(d, i):
        return pl.ds(ACC_Y + (d * N_OCC + i) * YR, YC)

    def v_y(i):
        return remote(pool.at[acc_x(1, i)], vy.at[i, live_x], v_send.at[0, i], v_recv.at[0, i], (frag, 1 - y, dev))

    def v_x(i):
        return remote(pool.at[acc_y(1, i)], vx.at[i, live], v_send.at[1, i], v_recv.at[1, i],
                      (frag, y, 2 * (1 - x) + core))

    def share(half):
        for i in range(half, half + 3):
            v_y(i).start()
            v_x(i).start()

    arrive(last)
    third(last, False, (1,), share)
    third(last, False, (0,))

    def sent(u, carry):
        for b in range(2):
            cross_x(u, b, b).wait_send()
            cross_y(u, b, b).wait_send()
        pair_x(u).wait_send()
        pair_y(u).wait_send()
        return carry

    lax.fori_loop(0, PAIRS, sent, 0)

    for i in range(N_OCC):
        v_y(i).wait_recv()
        out_ref[i, :XC] = (pool[acc_x(0, i), :] + vy[i, :XC])[:, :N_VIR]
        v_x(i).wait_recv()
        out_ref[i, XC:] = (pool[acc_y(0, i), :] + vx[i, :YC])[:, :N_VIR]
    for i in range(N_OCC):
        v_y(i).wait_send()
        v_x(i).wait_send()


def solution(mesh):
    def local_program(ints_blk, c_occ, c_vir):
        dma = pltpu.SemaphoreType.DMA
        xb, yb = (2, XR, 128), (2, YR, 128)
        out = pl.pallas_call(
            kernel,
            out_shape=jax.ShapeDtypeStruct((N_OCC, COLS, N_VIR), F32),
            in_specs=[pl.BlockSpec(memory_space=pl.ANY)] * 3,
            out_specs=pl.BlockSpec(memory_space=pltpu.VMEM),
            scratch_shapes=[
                pltpu.VMEM((N_OCC, N_R), BF16),
                pltpu.VMEM((N_VIR, N_R), BF16),
                pltpu.VMEM((SLOTS, N_Q, 120, N_R), BF16),
                pltpu.VMEM((8, 8 * N_OCC, 120), BF16),
                pltpu.VMEM((2, 2 * (XR + YR), 256), BF16),
                pltpu.VMEM((256, 256), BF16),
                pltpu.VMEM((N_OCC * 120, 128), F32),
                pltpu.VMEM((2, N_OCC, 128, 128), BF16),
                pltpu.VMEM((PAIRS, 2) + xb, BF16),
                pltpu.VMEM((PAIRS, 2) + yb, BF16),
                pltpu.VMEM((PAIRS, 2) + xb, BF16),
                pltpu.VMEM((PAIRS, 2) + yb, BF16),
                pltpu.VMEM((PAIRS,) + xb, BF16),
                pltpu.VMEM((PAIRS,) + yb, BF16),
                pltpu.VMEM((PAIRS, 2) + xb, BF16),
                pltpu.VMEM((PAIRS, 2) + yb, BF16),
                pltpu.VMEM((COEF + N_OCC * 120, 128), F32),
                pltpu.VMEM((N_OCC, YR, 128), F32),
                pltpu.VMEM((N_OCC, XR, 128), F32),
                dma((SLOTS,)), dma((2,)), dma((PAIRS, 6)), dma((PAIRS, 6)),
                dma((2, N_OCC)), dma((2, N_OCC)),
            ],
            compiler_params=pltpu.CompilerParams(
                collective_id=0, has_side_effects=True,
                vmem_limit_bytes=36 * 1024 * 1024),
        )(ints_blk, pltpu.with_memory_space_constraint(c_occ.T, pltpu.HBM),
          pltpu.with_memory_space_constraint(c_vir.T, pltpu.HBM))
        return jnp.transpose(out, (0, 2, 1))

    return jax.shard_map(
        local_program,
        mesh=mesh,
        in_specs=(P(('frag', 'dev'), 'dev2', None, None), P('frag', None), P('frag', None)),
        out_specs=P(None, None, ('frag', 'dev2', 'dev')),
        check_vma=False,
    )
```

```python
import jax
import jax.numpy as jnp
from jax import lax
from jax.experimental import pallas as pl
from jax.experimental.pallas import tpu as pltpu
from jax.sharding import PartitionSpec as P

MESH = pl.DeviceIdType.MESH
F32 = jnp.float32
BF16 = jnp.bfloat16

N_P = 29
N_Q = 58
HALF = 29
N_R = 116
N_OCC = 6
N_VIR = 112
COLS = 84
XC = 42
YC = 42
XR = 48
YR = 48
SLOTS = 6
PAIRS = 15
ACC_X = 0
ACC_Y = ACC_X + 2 * N_OCC * XR
COEF = ACC_Y + 2 * N_OCC * YR
LAG = 8


def kernel(a_ref, cot_ref, cvt_ref, out_ref, cot_v, cvt_v, abuf, lhs1, w2, cvb, cob, t1,
           lx, ly, xs, ys, px, py, xr, yr, pool, vx, vy,
           a_sem, c_sem, send, recv, v_send, v_recv):
    frag = lax.axis_index("frag")
    y = lax.axis_index("dev2")
    dev = lax.axis_index("dev")
    x = dev // 2
    core = dev % 2
    partner = (frag, y, 2 * x + 1 - core)
    xnbr = [(frag, y, 2 * (1 - x) + b) for b in range(2)]
    ynbr = [(frag, 1 - y, 2 * x + b) for b in range(2)]

    small = [pltpu.make_async_copy(cot_ref, cot_v, c_sem.at[0]),
             pltpu.make_async_copy(cvt_ref, cvt_v, c_sem.at[1])]
    for copy in small:
        copy.start()

    def fetch(p, slot):
        return pltpu.make_async_copy(
            a_ref.at[p], abuf.at[slot, :, pl.ds(0, N_R)], a_sem.at[slot])

    for p in range(SLOTS):
        fetch(p, p).start()

    rest = jnp.zeros((PAIRS, 2, 2, YR - YC, 128), BF16)
    yr[:, :, :, YC:, :] = rest
    py[:, :, YC:, :] = rest[:, 0]
    rest = jnp.zeros((PAIRS, 2, 2, XR - XC, 128), BF16)
    xr[:, :, :, XC:, :] = rest
    px[:, :, XC:, :] = rest[:, 0]

    barrier = pltpu.get_barrier_semaphore()
    for peer in [partner] + xnbr + ynbr:
        pl.semaphore_signal(barrier, inc=1, device_id=peer, device_id_type=MESH)

    for s in range(SLOTS):
        abuf[s, :, N_R:, :] = jnp.zeros((N_Q, 4, N_R), BF16)
    pool[...] = jnp.zeros_like(pool)
    lhs1[...] = jnp.zeros_like(lhs1)
    w2[...] = jnp.zeros_like(w2)
    cvb[...] = jnp.zeros_like(cvb)
    cob[...] = jnp.zeros_like(cob)
    for copy in small:
        copy.wait()

    cot = cot_v[...].astype(F32)
    rep = jnp.concatenate(
        [jnp.broadcast_to(cot[j:j + 1], (8, N_R)) for j in range(N_OCC)], axis=0)
    sub = lax.broadcasted_iota(jnp.int32, (8 * N_OCC, N_R), 0) % 8
    for m in range(8):
        lhs1[m, :, :N_R] = jnp.where(sub == m, rep, 0.0).astype(BF16)

    def first(slot, par, k):
        sums = []
        for g in range(4):
            total = None
            for m in range(min(8, HALF - 8 * g)):
                q = 8 * g + m
                left = jnp.pad(abuf[slot, q], ((0, 0), (0, 12)))
                right = jnp.pad(abuf[slot, HALF + q], ((0, 0), (0, 12)))
                term = jnp.dot(lhs1[m], jnp.concatenate([left, right], axis=1),
                               preferred_element_type=F32)
                total = term if total is None else total + term
            sums.append(total)
        for gp in range(2):
            for j in range(N_OCC):
                for h in range(2):
                    both = jnp.concatenate(
                        [sums[2 * gp + e][8 * j:8 * j + 8, 128 * h:128 * h + 128] for e in range(2)],
                        axis=0)
                    t1[par, j, k * 64 + h * 32 + gp * 16:k * 64 + h * 32 + gp * 16 + 16, :] = (
                        both.astype(BF16))

    def refill(p):
        @pl.when(p + SLOTS < N_P)
        def _():
            fetch(p + SLOTS, p % SLOTS).start()

    t1[...] = jnp.zeros_like(t1)
    fetch(0, 0).wait()
    first(0, 0, 1)
    refill(0)

    cvt = cvt_v[...].astype(F32)

    def put(xt, b, pieces):
        for kk in (0, 1):
            rows = jnp.concatenate(
                [cvt[lo:lo + n] if k == kk else jnp.zeros((n, N_R), F32) for n, lo, k in pieces]
                + [jnp.zeros((YR - YC, N_R), F32)], axis=0)
            head = jnp.concatenate([rows[:XC], jnp.zeros((XR - XC, N_R), F32)], axis=0)
            w2[xt, b * XR:(b + 1) * XR, kk * 128:kk * 128 + N_R] = head.astype(BF16)
            w2[xt, 2 * XR + b * YR:2 * XR + (b + 1) * YR, kk * 128:kk * 128 + N_R] = (
                rows[XC:].astype(BF16))

    put(0, 0, [(84, 0, 0)])
    put(0, 1, [(28, 84, 0), (56, 0, 1)])
    put(1, 0, [(56, 56, 0), (28, 0, 1)])
    put(1, 1, [(84, 28, 1)])

    cv = cvt.T
    for side in range(2):
        for h in range(2):
            lo = h * HALF
            low, high = cv[lo:lo + HALF], cv[N_Q + lo:N_Q + lo + HALF]
            part = jnp.where(y == side, low, high)
            part = jnp.concatenate([part, jnp.zeros((3, N_VIR), F32)], axis=0).astype(BF16)
            for k in range(2):
                cvb[pl.ds(side * 128 + k * 64 + h * 32, 32), k * 128:k * 128 + N_VIR] = part

    co = cot.T
    for i in range(N_OCC):
        rows = jnp.broadcast_to(co[:, i:i + 1], (N_R, 128))
        cob[i * 120 + 1:i * 120 + 1 + N_R, :] = rows
        pool[COEF + i * 120 + 1:COEF + i * 120 + 1 + N_R, :] = rows

    def second(u, par):
        for dx in range(2):
            xt = (x + dx) % 2
            rows = []
            for dy in range(2):
                j0 = 3 * ((y + dy) % 2) + xt
                rows.append(jnp.concatenate([t1[par, j0], t1[par, j0 + 1]], axis=1))
            half = lax.dot_general(w2[xt], jnp.concatenate(rows, axis=0), (((1,), (1,)), ((), ())),
                                   preferred_element_type=F32).astype(BF16)
            for b in range(2):
                for dy in range(2):
                    lane = slice(128 * dy, 128 * dy + 128)
                    (lx, xs)[dx][u, b, dy] = half[b * XR:(b + 1) * XR, lane]
                    (ly, ys)[dy][u, b, dx] = half[2 * XR + b * YR:2 * XR + (b + 1) * YR, lane]

    def remote(src, dst, s, r, peer):
        return pltpu.make_async_remote_copy(
            src_ref=src, dst_ref=dst, send_sem=s, recv_sem=r, device_id=peer, device_id_type=MESH)

    live_x, live = pl.ds(0, XC), pl.ds(0, YC)

    def cross_x(u, b, mark):
        return remote(xs.at[u, b, :, live_x], xr.at[u, core, :, live_x], send.at[u, b],
                      recv.at[u, mark], xnbr[b])

    def cross_y(u, b, mark):
        return remote(ys.at[u, b, :, live], yr.at[u, core, :, live], send.at[u, 2 + b],
                      recv.at[u, 2 + mark], ynbr[b])

    def pair_x(u):
        return remote(lx.at[u, 1 - core, :, live_x], px.at[u, :, live_x], send.at[u, 4],
                      recv.at[u, 4], partner)

    def pair_y(u):
        return remote(ly.at[u, 1 - core, :, live], py.at[u, :, live], send.at[u, 5],
                      recv.at[u, 5], partner)

    def send_pair(u):
        for b in range(2):
            cross_y(u, b, core).start()
            cross_x(u, b, core).start()
        pair_x(u).start()
        pair_y(u).start()

    def arrive(u):
        for b in range(2):
            cross_x(u, b, b).wait_recv()
            cross_y(u, b, b).wait_recv()
        pair_x(u).wait_recv()
        pair_y(u).wait_recv()

    def scales(u, source, table, base):
        p = source * N_P + 2 * u
        return [[jnp.broadcast_to(table[pl.ds(base + i * 120 + p + e, 1), :], (8, 128))
                 for i in range(N_OCC)] for e in range(2)]

    def gather(base, tiles, g, source, u, half, paced):
        for lo, hi in ((0, tiles // 2), (tiles // 2, tiles)) if paced else ((0, tiles),):
            table, at = (pool, COEF) if paced else (cob, 0)
            scale = [scales(u, s, table, at) for s in source]
            for r in range(lo, hi):
                for i in range(half, half + 3):
                    row = base + i * tiles * 8 + 8 * r
                    v = pool[row:row + 8, :]
                    for rows, sc in zip(g, scale):
                        for e in range(2):
                            v = v + sc[e][i] * rows[8 * r:8 * r + 8, 128 * e:128 * e + 128]
                    pool[row:row + 8, :] = v

    from_x = [dev, 2 * x + 1 - core, 2 * (1 - x), 2 * (1 - x) + 1]

    def third(u, paced, order=(0, 1), between=None):
        flat = [lx[u, core], px[u], xr[u, 0], xr[u, 1]]
        ys_in = [jnp.concatenate([ly[u, core], yr[u, core]], axis=2),
                 jnp.concatenate([py[u], yr[u, 1 - core]], axis=2)]
        gx = jnp.dot(jnp.concatenate([f[d] for d in order for f in flat], axis=0), cvb[:128],
                     preferred_element_type=F32)
        gy = jnp.dot(jnp.concatenate([f[d] for d in order for f in ys_in], axis=0), cvb[...],
                     preferred_element_type=F32)
        for n, d in enumerate(order):
            for half in (0, 3):
                for s in range(0, 4, 2):
                    at = (len(flat) * n + s) * XR
                    gather(ACC_X + d * N_OCC * XR, XR // 8,
                           [gx[at:at + XR], gx[at + XR:at + 2 * XR]], from_x[s:s + 2], u, half, paced)
                at = 2 * n * YR
                gather(ACC_Y + d * N_OCC * YR, YR // 8,
                       [gy[at:at + YR], gy[at + YR:at + 2 * YR]], from_x[:2], u, half, paced)
                if between is not None:
                    between(half)


    def stream(u):
        fetch(2 * u - 1, (2 * u - 1) % SLOTS).wait()
        fetch(2 * u, 2 * u % SLOTS).wait()

    def trip(u, before=True):
        first((2 * u - 1) % SLOTS, u % 2, 0)
        first(2 * u % SLOTS, u % 2, 1)
        if before:
            send_pair(u - 1)
        refill(2 * u - 1)
        refill(2 * u)

    pl.semaphore_wait(barrier, 5)
    second(0, 0)
    send_pair(0)
    stream(1)
    trip(1, False)

    def early(u, carry):
        stream(u)
        second(u - 1, (u + 1) % 2)
        trip(u)
        return carry

    def late(u, carry):
        stream(u)
        arrive(u - LAG)
        third(u - LAG, True)
        second(u - 1, (u + 1) % 2)
        trip(u)
        return carry

    last = PAIRS - 1
    lax.fori_loop(2, LAG, early, 0)
    lax.fori_loop(LAG, last, late, 0)
    second(last - 1, (last - 1) % 2)
    send_pair(last - 1)
    p = 2 * last - 1
    stream(last)
    first(p % SLOTS, last % 2, 0)
    first((p + 1) % SLOTS, last % 2, 1)
    second(last, last % 2)
    send_pair(last)

    def drain(n, carry):
        u = last - LAG + 2 * n
        arrive(u)
        arrive(u + 1)
        third(u, False)
        third(u + 1, False)
        return carry

    lax.fori_loop(0, LAG // 2, drain, 0)
    def acc_x(d, i):
        return pl.ds(ACC_X + (d * N_OCC + i) * XR, XC)

    def acc_y(d, i):
        return pl.ds(ACC_Y + (d * N_OCC + i) * YR, YC)

    def v_y(i):
        return remote(pool.at[acc_x(1, i)], vy.at[i, live_x], v_send.at[0, i], v_recv.at[0, i], (frag, 1 - y, dev))

    def v_x(i):
        return remote(pool.at[acc_y(1, i)], vx.at[i, live], v_send.at[1, i], v_recv.at[1, i],
                      (frag, y, 2 * (1 - x) + core))

    def share(half):
        for i in range(half, half + 3):
            v_y(i).start()
            v_x(i).start()

    arrive(last)
    third(last, False, (1,), share)
    third(last, False, (0,))

    def sent(u, carry):
        for b in range(2):
            cross_x(u, b, b).wait_send()
            cross_y(u, b, b).wait_send()
        pair_x(u).wait_send()
        pair_y(u).wait_send()
        return carry

    lax.fori_loop(0, PAIRS, sent, 0)

    for i in range(N_OCC):
        v_y(i).wait_recv()
        out_ref[i, :XC] = (pool[acc_x(0, i), :] + vy[i, :XC])[:, :N_VIR]
        v_x(i).wait_recv()
        out_ref[i, XC:] = (pool[acc_y(0, i), :] + vx[i, :YC])[:, :N_VIR]
    for i in range(N_OCC):
        v_y(i).wait_send()
        v_x(i).wait_send()


def solution(mesh):
    def local_program(ints_blk, c_occ, c_vir):
        dma = pltpu.SemaphoreType.DMA
        xb, yb = (2, XR, 128), (2, YR, 128)
        out = pl.pallas_call(
            kernel,
            out_shape=jax.ShapeDtypeStruct((N_OCC, COLS, N_VIR), F32),
            in_specs=[pl.BlockSpec(memory_space=pl.ANY)] * 3,
            out_specs=pl.BlockSpec(memory_space=pltpu.VMEM),
            scratch_shapes=[
                pltpu.VMEM((N_OCC, N_R), BF16),
                pltpu.VMEM((N_VIR, N_R), BF16),
                pltpu.VMEM((SLOTS, N_Q, 120, N_R), BF16),
                pltpu.VMEM((8, 8 * N_OCC, 120), BF16),
                pltpu.VMEM((2, 2 * (XR + YR), 256), BF16),
                pltpu.VMEM((256, 256), BF16),
                pltpu.VMEM((N_OCC * 120, 128), F32),
                pltpu.VMEM((2, N_OCC, 128, 128), BF16),
                pltpu.VMEM((PAIRS, 2) + xb, BF16),
                pltpu.VMEM((PAIRS, 2) + yb, BF16),
                pltpu.VMEM((PAIRS, 2) + xb, BF16),
                pltpu.VMEM((PAIRS, 2) + yb, BF16),
                pltpu.VMEM((PAIRS,) + xb, BF16),
                pltpu.VMEM((PAIRS,) + yb, BF16),
                pltpu.VMEM((PAIRS, 2) + xb, BF16),
                pltpu.VMEM((PAIRS, 2) + yb, BF16),
                pltpu.VMEM((COEF + N_OCC * 120, 128), F32),
                pltpu.VMEM((N_OCC, YR, 128), F32),
                pltpu.VMEM((N_OCC, XR, 128), F32),
                dma((SLOTS,)), dma((2,)), dma((PAIRS, 6)), dma((PAIRS, 6)),
                dma((2, N_OCC)), dma((2, N_OCC)),
            ],
            compiler_params=pltpu.CompilerParams(
                collective_id=0, has_side_effects=True,
                vmem_limit_bytes=36 * 1024 * 1024),
        )(ints_blk, pltpu.with_memory_space_constraint(c_occ.T, pltpu.HBM),
          pltpu.with_memory_space_constraint(c_vir.T, pltpu.HBM))
        return jnp.transpose(out, (0, 2, 1))

    return jax.shard_map(
        local_program,
        mesh=mesh,
        in_specs=(P(('frag', 'dev'), 'dev2', None, None), P('frag', None), P('frag', None)),
        out_specs=P(None, None, ('frag', 'dev2', 'dev')),
        check_vma=False,
    )
```

```python
import jax
import jax.numpy as jnp
from jax import lax
from jax.experimental import pallas as pl
from jax.experimental.pallas import tpu as pltpu
from jax.sharding import PartitionSpec as P

MESH = pl.DeviceIdType.MESH
F32 = jnp.float32
BF16 = jnp.bfloat16

N_P = 29
N_Q = 58
HALF = 29
N_R = 116
N_OCC = 6
N_VIR = 112
COLS = 84
XC = 42
YC = 42
XR = 48
YR = 48
SLOTS = 6
PAIRS = 15
ACC_X = 0
ACC_Y = ACC_X + 2 * N_OCC * XR
COEF = ACC_Y + 2 * N_OCC * YR
LAG = 10


def kernel(a_ref, cot_ref, cvt_ref, out_ref, cot_v, cvt_v, abuf, lhs1, w2, cvb, cob, t1,
           lx, ly, xs, ys, px, py, xr, yr, pool, vx, vy,
           a_sem, c_sem, send, recv, v_send, v_recv):
    frag = lax.axis_index("frag")
    y = lax.axis_index("dev2")
    dev = lax.axis_index("dev")
    x = dev // 2
    core = dev % 2
    partner = (frag, y, 2 * x + 1 - core)
    xnbr = [(frag, y, 2 * (1 - x) + b) for b in range(2)]
    ynbr = [(frag, 1 - y, 2 * x + b) for b in range(2)]

    small = [pltpu.make_async_copy(cot_ref, cot_v, c_sem.at[0]),
             pltpu.make_async_copy(cvt_ref, cvt_v, c_sem.at[1])]
    for copy in small:
        copy.start()

    def fetch(p, slot):
        return pltpu.make_async_copy(
            a_ref.at[p], abuf.at[slot, :, pl.ds(0, N_R)], a_sem.at[slot])

    for p in range(SLOTS):
        fetch(p, p).start()

    rest = jnp.zeros((PAIRS, 2, 2, YR - YC, 128), BF16)
    yr[:, :, :, YC:, :] = rest
    py[:, :, YC:, :] = rest[:, 0]
    rest = jnp.zeros((PAIRS, 2, 2, XR - XC, 128), BF16)
    xr[:, :, :, XC:, :] = rest
    px[:, :, XC:, :] = rest[:, 0]

    barrier = pltpu.get_barrier_semaphore()
    for peer in [partner] + xnbr + ynbr:
        pl.semaphore_signal(barrier, inc=1, device_id=peer, device_id_type=MESH)

    for s in range(SLOTS):
        abuf[s, :, N_R:, :] = jnp.zeros((N_Q, 4, N_R), BF16)
    pool[...] = jnp.zeros_like(pool)
    lhs1[...] = jnp.zeros_like(lhs1)
    w2[...] = jnp.zeros_like(w2)
    cvb[...] = jnp.zeros_like(cvb)
    cob[...] = jnp.zeros_like(cob)
    for copy in small:
        copy.wait()

    cot = cot_v[...].astype(F32)
    rep = jnp.concatenate(
        [jnp.broadcast_to(cot[j:j + 1], (8, N_R)) for j in range(N_OCC)], axis=0)
    sub = lax.broadcasted_iota(jnp.int32, (8 * N_OCC, N_R), 0) % 8
    for m in range(8):
        lhs1[m, :, :N_R] = jnp.where(sub == m, rep, 0.0).astype(BF16)

    def first(slot, par, k):
        sums = []
        for g in range(4):
            total = None
            for m in range(min(8, HALF - 8 * g)):
                q = 8 * g + m
                left = jnp.pad(abuf[slot, q], ((0, 0), (0, 12)))
                right = jnp.pad(abuf[slot, HALF + q], ((0, 0), (0, 12)))
                term = jnp.dot(lhs1[m], jnp.concatenate([left, right], axis=1),
                               preferred_element_type=F32)
                total = term if total is None else total + term
            sums.append(total)
        for gp in range(2):
            for j in range(N_OCC):
                for h in range(2):
                    both = jnp.concatenate(
                        [sums[2 * gp + e][8 * j:8 * j + 8, 128 * h:128 * h + 128] for e in range(2)],
                        axis=0)
                    t1[par, j, k * 64 + h * 32 + gp * 16:k * 64 + h * 32 + gp * 16 + 16, :] = (
                        both.astype(BF16))

    def refill(p):
        @pl.when(p + SLOTS < N_P)
        def _():
            fetch(p + SLOTS, p % SLOTS).start()

    t1[...] = jnp.zeros_like(t1)
    fetch(0, 0).wait()
    first(0, 0, 1)
    refill(0)

    cvt = cvt_v[...].astype(F32)

    def put(xt, b, pieces):
        for kk in (0, 1):
            rows = jnp.concatenate(
                [cvt[lo:lo + n] if k == kk else jnp.zeros((n, N_R), F32) for n, lo, k in pieces]
                + [jnp.zeros((YR - YC, N_R), F32)], axis=0)
            head = jnp.concatenate([rows[:XC], jnp.zeros((XR - XC, N_R), F32)], axis=0)
            w2[xt, b * XR:(b + 1) * XR, kk * 128:kk * 128 + N_R] = head.astype(BF16)
            w2[xt, 2 * XR + b * YR:2 * XR + (b + 1) * YR, kk * 128:kk * 128 + N_R] = (
                rows[XC:].astype(BF16))

    put(0, 0, [(84, 0, 0)])
    put(0, 1, [(28, 84, 0), (56, 0, 1)])
    put(1, 0, [(56, 56, 0), (28, 0, 1)])
    put(1, 1, [(84, 28, 1)])

    cv = cvt.T
    for side in range(2):
        for h in range(2):
            lo = h * HALF
            low, high = cv[lo:lo + HALF], cv[N_Q + lo:N_Q + lo + HALF]
            part = jnp.where(y == side, low, high)
            part = jnp.concatenate([part, jnp.zeros((3, N_VIR), F32)], axis=0).astype(BF16)
            for k in range(2):
                cvb[pl.ds(side * 128 + k * 64 + h * 32, 32), k * 128:k * 128 + N_VIR] = part

    co = cot.T
    for i in range(N_OCC):
        rows = jnp.broadcast_to(co[:, i:i + 1], (N_R, 128))
        cob[i * 120 + 1:i * 120 + 1 + N_R, :] = rows
        pool[COEF + i * 120 + 1:COEF + i * 120 + 1 + N_R, :] = rows

    def second(u, par):
        for dx in range(2):
            xt = (x + dx) % 2
            rows = []
            for dy in range(2):
                j0 = 3 * ((y + dy) % 2) + xt
                rows.append(jnp.concatenate([t1[par, j0], t1[par, j0 + 1]], axis=1))
            half = lax.dot_general(w2[xt], jnp.concatenate(rows, axis=0), (((1,), (1,)), ((), ())),
                                   preferred_element_type=F32).astype(BF16)
            for b in range(2):
                for dy in range(2):
                    lane = slice(128 * dy, 128 * dy + 128)
                    (lx, xs)[dx][u, b, dy] = half[b * XR:(b + 1) * XR, lane]
                    (ly, ys)[dy][u, b, dx] = half[2 * XR + b * YR:2 * XR + (b + 1) * YR, lane]

    def remote(src, dst, s, r, peer):
        return pltpu.make_async_remote_copy(
            src_ref=src, dst_ref=dst, send_sem=s, recv_sem=r, device_id=peer, device_id_type=MESH)

    live_x, live = pl.ds(0, XC), pl.ds(0, YC)

    def cross_x(u, b, mark):
        return remote(xs.at[u, b, :, live_x], xr.at[u, core, :, live_x], send.at[u, b],
                      recv.at[u, mark], xnbr[b])

    def cross_y(u, b, mark):
        return remote(ys.at[u, b, :, live], yr.at[u, core, :, live], send.at[u, 2 + b],
                      recv.at[u, 2 + mark], ynbr[b])

    def pair_x(u):
        return remote(lx.at[u, 1 - core, :, live_x], px.at[u, :, live_x], send.at[u, 4],
                      recv.at[u, 4], partner)

    def pair_y(u):
        return remote(ly.at[u, 1 - core, :, live], py.at[u, :, live], send.at[u, 5],
                      recv.at[u, 5], partner)

    def send_pair(u):
        for b in range(2):
            cross_y(u, b, core).start()
            cross_x(u, b, core).start()
        pair_x(u).start()
        pair_y(u).start()

    def arrive(u):
        for b in range(2):
            cross_x(u, b, b).wait_recv()
            cross_y(u, b, b).wait_recv()
        pair_x(u).wait_recv()
        pair_y(u).wait_recv()

    def scales(u, source, table, base):
        p = source * N_P + 2 * u
        return [[jnp.broadcast_to(table[pl.ds(base + i * 120 + p + e, 1), :], (8, 128))
                 for i in range(N_OCC)] for e in range(2)]

    def gather(base, tiles, g, source, u, half, paced):
        for lo, hi in ((0, tiles // 2), (tiles // 2, tiles)) if paced else ((0, tiles),):
            table, at = (pool, COEF) if paced else (cob, 0)
            scale = [scales(u, s, table, at) for s in source]
            for r in range(lo, hi):
                for i in range(half, half + 3):
                    row = base + i * tiles * 8 + 8 * r
                    v = pool[row:row + 8, :]
                    for rows, sc in zip(g, scale):
                        for e in range(2):
                            v = v + sc[e][i] * rows[8 * r:8 * r + 8, 128 * e:128 * e + 128]
                    pool[row:row + 8, :] = v

    from_x = [dev, 2 * x + 1 - core, 2 * (1 - x), 2 * (1 - x) + 1]

    def third(u, paced, order=(0, 1), between=None):
        flat = [lx[u, core], px[u], xr[u, 0], xr[u, 1]]
        ys_in = [jnp.concatenate([ly[u, core], yr[u, core]], axis=2),
                 jnp.concatenate([py[u], yr[u, 1 - core]], axis=2)]
        gx = jnp.dot(jnp.concatenate([f[d] for d in order for f in flat], axis=0), cvb[:128],
                     preferred_element_type=F32)
        gy = jnp.dot(jnp.concatenate([f[d] for d in order for f in ys_in], axis=0), cvb[...],
                     preferred_element_type=F32)
        for n, d in enumerate(order):
            for half in (0, 3):
                for s in range(0, 4, 2):
                    at = (len(flat) * n + s) * XR
                    gather(ACC_X + d * N_OCC * XR, XR // 8,
                           [gx[at:at + XR], gx[at + XR:at + 2 * XR]], from_x[s:s + 2], u, half, paced)
                at = 2 * n * YR
                gather(ACC_Y + d * N_OCC * YR, YR // 8,
                       [gy[at:at + YR], gy[at + YR:at + 2 * YR]], from_x[:2], u, half, paced)
                if between is not None:
                    between(half)


    def stream(u):
        fetch(2 * u - 1, (2 * u - 1) % SLOTS).wait()
        fetch(2 * u, 2 * u % SLOTS).wait()

    def trip(u, before=True):
        first((2 * u - 1) % SLOTS, u % 2, 0)
        first(2 * u % SLOTS, u % 2, 1)
        if before:
            send_pair(u - 1)
        refill(2 * u - 1)
        refill(2 * u)

    pl.semaphore_wait(barrier, 5)
    second(0, 0)
    send_pair(0)
    stream(1)
    trip(1, False)

    def early(u, carry):
        stream(u)
        second(u - 1, (u + 1) % 2)
        trip(u)
        return carry

    def late(u, carry):
        stream(u)
        arrive(u - LAG)
        third(u - LAG, True)
        second(u - 1, (u + 1) % 2)
        trip(u)
        return carry

    last = PAIRS - 1
    lax.fori_loop(2, LAG, early, 0)
    lax.fori_loop(LAG, last, late, 0)
    second(last - 1, (last - 1) % 2)
    send_pair(last - 1)
    p = 2 * last - 1
    stream(last)
    first(p % SLOTS, last % 2, 0)
    first((p + 1) % SLOTS, last % 2, 1)
    second(last, last % 2)
    send_pair(last)

    def drain(n, carry):
        u = last - LAG + 3 * n
        for k in range(3):
            arrive(u + k)
        for k in range(3):
            third(u + k, False)
        return carry

    lax.fori_loop(0, LAG // 3, drain, 0)

    def acc_x(d, i):
        return pl.ds(ACC_X + (d * N_OCC + i) * XR, XC)

    def acc_y(d, i):
        return pl.ds(ACC_Y + (d * N_OCC + i) * YR, YC)

    def v_y(i):
        return remote(pool.at[acc_x(1, i)], vy.at[i, live_x], v_send.at[0, i], v_recv.at[0, i], (frag, 1 - y, dev))

    def v_x(i):
        return remote(pool.at[acc_y(1, i)], vx.at[i, live], v_send.at[1, i], v_recv.at[1, i],
                      (frag, y, 2 * (1 - x) + core))

    def share(half):
        for i in range(half, half + 3):
            v_y(i).start()
            v_x(i).start()

    arrive(last - 1)
    arrive(last)
    third(last - 1, False)
    third(last, False, (1,), share)
    third(last, False, (0,))

    def sent(u, carry):
        for b in range(2):
            cross_x(u, b, b).wait_send()
            cross_y(u, b, b).wait_send()
        pair_x(u).wait_send()
        pair_y(u).wait_send()
        return carry

    lax.fori_loop(0, PAIRS, sent, 0)

    for i in range(N_OCC):
        v_y(i).wait_recv()
        out_ref[i, :XC] = (pool[acc_x(0, i), :] + vy[i, :XC])[:, :N_VIR]
        v_x(i).wait_recv()
        out_ref[i, XC:] = (pool[acc_y(0, i), :] + vx[i, :YC])[:, :N_VIR]
    for i in range(N_OCC):
        v_y(i).wait_send()
        v_x(i).wait_send()


def solution(mesh):
    def local_program(ints_blk, c_occ, c_vir):
        dma = pltpu.SemaphoreType.DMA
        xb, yb = (2, XR, 128), (2, YR, 128)
        out = pl.pallas_call(
            kernel,
            out_shape=jax.ShapeDtypeStruct((N_OCC, COLS, N_VIR), F32),
            in_specs=[pl.BlockSpec(memory_space=pl.ANY)] * 3,
            out_specs=pl.BlockSpec(memory_space=pltpu.VMEM),
            scratch_shapes=[
                pltpu.VMEM((N_OCC, N_R), BF16),
                pltpu.VMEM((N_VIR, N_R), BF16),
                pltpu.VMEM((SLOTS, N_Q, 120, N_R), BF16),
                pltpu.VMEM((8, 8 * N_OCC, 120), BF16),
                pltpu.VMEM((2, 2 * (XR + YR), 256), BF16),
                pltpu.VMEM((256, 256), BF16),
                pltpu.VMEM((N_OCC * 120, 128), F32),
                pltpu.VMEM((2, N_OCC, 128, 128), BF16),
                pltpu.VMEM((PAIRS, 2) + xb, BF16),
                pltpu.VMEM((PAIRS, 2) + yb, BF16),
                pltpu.VMEM((PAIRS, 2) + xb, BF16),
                pltpu.VMEM((PAIRS, 2) + yb, BF16),
                pltpu.VMEM((PAIRS,) + xb, BF16),
                pltpu.VMEM((PAIRS,) + yb, BF16),
                pltpu.VMEM((PAIRS, 2) + xb, BF16),
                pltpu.VMEM((PAIRS, 2) + yb, BF16),
                pltpu.VMEM((COEF + N_OCC * 120, 128), F32),
                pltpu.VMEM((N_OCC, YR, 128), F32),
                pltpu.VMEM((N_OCC, XR, 128), F32),
                dma((SLOTS,)), dma((2,)), dma((PAIRS, 6)), dma((PAIRS, 6)),
                dma((2, N_OCC)), dma((2, N_OCC)),
            ],
            compiler_params=pltpu.CompilerParams(
                collective_id=0, has_side_effects=True,
                vmem_limit_bytes=36 * 1024 * 1024),
        )(ints_blk, pltpu.with_memory_space_constraint(c_occ.T, pltpu.HBM),
          pltpu.with_memory_space_constraint(c_vir.T, pltpu.HBM))
        return jnp.transpose(out, (0, 2, 1))

    return jax.shard_map(
        local_program,
        mesh=mesh,
        in_specs=(P(('frag', 'dev'), 'dev2', None, None), P('frag', None), P('frag', None)),
        out_specs=P(None, None, ('frag', 'dev2', 'dev')),
        check_vma=False,
    )
```
